512 devices in a mesh: crops: 2 (over y), dap: 64 (over z, core), chan: 4 (over x).
Axes of the slice: x: 4, y: 2, z: 32, core: 2. Of those that a mesh axis runs over, the one named last changes fastest.
The devices are a block of a 4x8x32 slice.
Arguments:
- prior_pair: bfloat16 [512, 256, 128], P(('crops', 'dap')), parts along dimension 0, may hold values from -12 to 12
- single: bfloat16 [512, 384], P(('crops', 'dap')), parts along dimension 0, may hold values from -6 to 6
- target: int32 [512], P(('crops', 'dap')), parts along dimension 0, may hold values from 0 to 21
- residue_mask: int32 [512], P(('crops', 'dap')), parts along dimension 0, may hold values 0 or 1
- recycle_gain: float32 [128], replicated, may hold values from 0.5 to 1.5
- recycle_bias: float32 [128], replicated, may hold values from -3 to 3
- left_single: bfloat16 [384, 128], replicated, may hold values from -0.3125 to 0.3125
- right_single: bfloat16 [384, 128], replicated, may hold values from -0.3125 to 0.3125
- left_target: bfloat16 [22, 128], replicated, may hold values from -3 to 3
- right_target: bfloat16 [22, 128], replicated, may hold values from -3 to 3
- tri_gain: float32 [2, 128], replicated, may hold values from 0.25 to 1.75
- tri_proj: bfloat16 [2, 128, 4, 128], replicated, may hold values from -0.5 to 0.5
- tri_gate: bfloat16 [2, 128, 128], replicated, may hold values from -0.5 to 0.5
- tri_gate_bias: float32 [2, 128], replicated, may hold values from -4 to 4
- tri_out_gain: float32 [2, 128], replicated, may hold values from 0.25 to 1.75
- tri_out: bfloat16 [2, 128, 128], replicated, may hold values from -0.5 to 0.5
Outputs:
- updated_pair: bfloat16 [512, 256, 128], P(('crops', 'dap')), parts along dimension 0
The draws below stay inside these ranges and needn't reach their ends.
There are 2 independent parts, one for each index of `crops`. The reference program is written for one: setup_inputs(seed, part) draws one part's arguments, and reference() takes and returns one part's arrays. A program takes and returns all parts, laid end to end along the dimension named above; an argument that names none is the same for every part. Nothing has to cross between parts.
All inputs are finite; a program needn't handle non-finite values. No bound on the sum of `residue_mask` on one device may be relied on, other than what follows from the above.
Results may differ from the reference program's by a relative error of at most 0.0085.
Values may be sent and summed in bfloat16 or wider, within the bound.
A program may use at most 64 MiB of HBM per device.

```python
import jax
import jax.numpy as jnp
from jax import lax

C_Z = 128
C_H = 128
C_S = 384
C_T = 22
N_RES = 256


def plant(values, key, least, high):
    extent = values.shape
    index_at = [jax.random.randint(jax.random.fold_in(key, axis), (), 0, extent[axis]) for axis in range(len(extent))]
    values = values.at[tuple(index_at)].set(least)
    longest = extent.index(max(extent))
    index_at[longest] = (index_at[longest] + 1) % extent[longest]
    return values.at[tuple(index_at)].set(high)


def block_scale(key, dims, pieces, least, high):
    loudness = 1.0
    for position, parts in pieces:
        steps = jax.random.uniform(jax.random.fold_in(jax.random.fold_in(key, 6), position), (parts,), jnp.float32, least / len(pieces), high / len(pieces))
        loudness = loudness * jnp.repeat(jnp.exp(steps), dims[position] // parts).reshape((-1,) + (1,) * (len(dims) - 1 - position))
    return loudness


def scatter_about(own_key, extent, scale, bound, cuts=(), kind=jnp.bfloat16):
    array = scale * jax.random.normal(own_key, extent, jnp.float32)
    if cuts:
        array = array * block_scale(own_key, extent, cuts, -0.22, 0.18)
    return jnp.clip(array, -bound, bound).astype(kind)


def setup_inputs(seed: int = 0, part: int = 0) -> dict:
    splits = jax.random.split(jax.random.key(seed), 17)
    part_splits = jax.random.split(jax.random.fold_in(splits[16], part), 17)
    return {
        "prior_pair": scatter_about(part_splits[0], (N_RES, N_RES, C_Z), 2.0, 12.0, ((0, 64),)),
        "single": scatter_about(part_splits[1], (N_RES, C_S), 1.0, 6.0, ((0, 64),)),
        "target": plant(jax.random.randint(part_splits[2], (N_RES,), 0, C_T), jax.random.fold_in(part_splits[2], 1), 0, C_T - 1).astype(jnp.int32),
        "residue_mask": plant((jax.random.randint(part_splits[3], (N_RES,), 0, 8) < 7).astype(jnp.int32), jax.random.fold_in(part_splits[3], 1), 0, 1),
        "recycle_gain": jnp.clip(1.0 + 0.1 * jax.random.normal(splits[4], (C_Z,), jnp.float32), 0.5, 1.5),
        "recycle_bias": scatter_about(splits[5], (C_Z,), 0.5, 3.0, (), jnp.float32),
        "left_single": scatter_about(splits[6], (C_S, C_Z), C_S ** -0.5, 0.3125),
        "right_single": scatter_about(splits[7], (C_S, C_Z), C_S ** -0.5, 0.3125),
        "left_target": scatter_about(splits[8], (C_T, C_Z), 0.5, 3.0),
        "right_target": scatter_about(splits[9], (C_T, C_Z), 0.5, 3.0),
        "tri_gain": jnp.clip(1.0 + 0.15 * jax.random.normal(splits[10], (2, C_Z), jnp.float32), 0.25, 1.75),
        "tri_proj": scatter_about(splits[11], (2, C_Z, 4, C_H), C_Z ** -0.5, 0.5),
        "tri_gate": scatter_about(splits[12], (2, C_Z, C_Z), C_Z ** -0.5, 0.5),
        "tri_gate_bias": scatter_about(splits[13], (2, C_Z), 1.0, 4.0, (), jnp.float32),
        "tri_out_gain": jnp.clip(1.0 + 0.15 * jax.random.normal(splits[14], (2, C_H), jnp.float32), 0.25, 1.75),
        "tri_out": scatter_about(splits[15], (2, C_H, C_Z), C_H ** -0.5, 0.5),
    }


def layer_norm(values, axis):
    center = values - lax.optimization_barrier(jnp.mean(values, axis=axis, keepdims=True))
    spread = lax.optimization_barrier(jnp.mean(center * center, axis=axis, keepdims=True))
    return center * lax.rsqrt(spread + 1e-05)

def reference(prior_pair, single, target, residue_mask, recycle_gain, recycle_bias, left_single, right_single, left_target, right_target, tri_gain, tri_proj, tri_gate, tri_gate_bias, tri_out_gain, tri_out):
    mask_float = residue_mask.astype(jnp.float32)
    pair_mask = mask_float[:, None] * mask_float[None, :]
    one_hot = (target[:, None] == jnp.arange(C_T, dtype=jnp.int32)[None, :]).astype(jnp.bfloat16)
    left_terms = jnp.dot(single, left_single, preferred_element_type=jnp.float32) + jnp.dot(one_hot, left_target, preferred_element_type=jnp.float32)
    right_terms = jnp.dot(single, right_single, preferred_element_type=jnp.float32) + jnp.dot(one_hot, right_target, preferred_element_type=jnp.float32)
    prior_norm = layer_norm(prior_pair.astype(jnp.float32), 2) * recycle_gain + recycle_bias
    pair_state = (prior_norm + left_terms[:, None, :] + right_terms[None, :, :]).astype(jnp.bfloat16)
    for layer in range(2):
        normed = (layer_norm(pair_state.astype(jnp.float32), 2) * tri_gain[layer]).astype(jnp.bfloat16)
        flat_normed = normed.reshape(-1, C_Z)
        projected = jnp.dot(flat_normed, tri_proj[layer].reshape(C_Z, 4 * C_H), preferred_element_type=jnp.float32).reshape(N_RES, N_RES, 4, C_H)
        masked = pair_mask[:, :, None]
        left_edges = (masked * jax.nn.sigmoid(projected[:, :, 1]) * projected[:, :, 0]).astype(jnp.bfloat16).astype(jnp.float32)
        right_edges = (masked * jax.nn.sigmoid(projected[:, :, 3]) * projected[:, :, 2]).astype(jnp.bfloat16).astype(jnp.float32)
        if layer == 0:
            product = jnp.einsum('ikc,jkc->ijc', left_edges, right_edges, precision=lax.Precision.HIGHEST)
        else:
            product = jnp.einsum('kic,kjc->ijc', left_edges, right_edges, precision=lax.Precision.HIGHEST)
        product = product.astype(jnp.bfloat16)
        normed_hidden = (layer_norm(product.astype(jnp.float32), 2) * tri_out_gain[layer]).astype(jnp.bfloat16)
        update = jnp.dot(normed_hidden.reshape(-1, C_H), tri_out[layer], preferred_element_type=jnp.float32)
        gating = jax.nn.sigmoid(jnp.dot(flat_normed, tri_gate[layer], preferred_element_type=jnp.float32) + tri_gate_bias[layer])
        pair_state = (pair_state.astype(jnp.float32) + (gating * update).reshape(N_RES, N_RES, C_Z)).astype(jnp.bfloat16)
    return pair_state
```

```python
import functools

import jax
import jax.numpy as jnp
from jax import lax
from jax.experimental import pallas as pl
from jax.experimental.pallas import tpu as pltpu
from jax.sharding import PartitionSpec as P

F32 = jnp.float32
BF16 = jnp.bfloat16
MESH = pl.DeviceIdType.MESH
EPS = 1e-05
LANES = 128


def selection(shape, column_of_row):
    rows = lax.broadcasted_iota(jnp.int32, shape, 0)
    columns = lax.broadcasted_iota(jnp.int32, shape, 1)
    return jnp.where(columns == column_of_row(rows), 1.0, 0.0).astype(BF16)


def nn(a, b):
    return lax.dot_general(a, b, (((1,), (0,)), ((), ())), preferred_element_type=F32)


def nt(a, b):
    return lax.dot_general(a, b, (((1,), (1,)), ((), ())), preferred_element_type=F32)


def norm_rows(values):
    scale = 1.0 / values.shape[0]
    center = values - jnp.sum(values, axis=0, keepdims=True) * scale
    spread = jnp.sum(center * center, axis=0, keepdims=True) * scale
    return center * lax.rsqrt(spread + EPS)


def column(row_vector):
    return jnp.transpose(jnp.broadcast_to(row_vector, (LANES, LANES)))


def kernel(
    rings,
    lanes_x,
    prior_ref,
    single_ref,
    target_ref,
    mask_ref,
    recycle_gain_ref,
    recycle_bias_ref,
    left_single_ref,
    right_single_ref,
    left_target_ref,
    right_target_ref,
    tri_gain_ref,
    tri_proj_ref,
    tri_gate_ref,
    tri_gate_bias_ref,
    tri_out_gain_ref,
    tri_out_ref,
    out_ref,
    terms,
    edges_out,
    left_in,
    right_in,
    product_out,
    product_in,
    base,
    pair,
    normed,
    weights,
    gate_weights,
    out_weights,
    columns,
    perm,
    perm_back,
    pick,
    pick_right,
    pick_left,
    terms_send,
    terms_recv,
    edge_send,
    edge_recv,
    back_send,
    back_recv,
    twin_send,
    twin_recv,
    lane_send,
    lane_recv,
):
    rows, cols, depth = prior_ref.shape
    blocks = rows * cols // LANES
    per_row = cols // LANES
    width = depth // lanes_x
    dap = lax.axis_index("dap")
    x = lax.axis_index("chan")
    z = dap // 2
    h = lax.rem(dap, 2)
    twin = {"dap": dap + 1 - 2 * h}

    def z_peer(t):
        up = (t + 1) // 2
        offset = rings // 2 + up * (1 - 2 * lax.rem(t + 1, 2))
        return lax.rem(z + offset, rings)

    def to_z(peer):
        return {"dap": 2 * peer + h}

    def to_x(t):
        return lax.rem(x + t, lanes_x)

    barrier = pltpu.get_barrier_semaphore()

    def greet(t, carry):
        pl.semaphore_signal(barrier, inc=1, device_id=to_z(z_peer(t)), device_id_type=MESH)
        return carry

    lax.fori_loop(0, rings - 1, greet, 0)
    pl.semaphore_signal(barrier, inc=1, device_id=twin, device_id_type=MESH)
    for t in range(1, lanes_x):
        pl.semaphore_signal(barrier, inc=1, device_id={"chan": to_x(t)}, device_id_type=MESH)

    single = single_ref[...]
    mask_of = [mask_ref[r].astype(F32) for r in range(rows)]

    def row_terms(weight_ref, table_ref):
        linear = nn(single, weight_ref[...])
        table = table_ref[...].astype(F32)
        classes = lax.broadcasted_iota(jnp.int32, table.shape, 0)
        picked = [
            jnp.sum(jnp.where(classes == target_ref[r], table, 0.0), axis=0, keepdims=True)
            for r in range(rows)
        ]
        return [linear[r : r + 1] + picked[r] for r in range(rows)]

    right_rows = row_terms(right_single_ref, right_target_ref)
    mask_rows = [jnp.full((1, depth), mask_of[r], F32) for r in range(rows)]
    tile = jnp.concatenate(right_rows + mask_rows, axis=0)
    terms[h, z] = jnp.where(h == 0, tile, pltpu.roll(tile, rows, 0))

    left_rows = row_terms(left_single_ref, left_target_ref)
    gain = recycle_gain_ref[...]
    bias = recycle_bias_ref[...]
    for r in range(rows):
        for jh in range(per_row):
            block = prior_ref[r, jh * LANES : (jh + 1) * LANES, :].astype(F32)
            center = block - jnp.mean(block, axis=1, keepdims=True)
            spread = jnp.mean(center * center, axis=1, keepdims=True)
            value = center * lax.rsqrt(spread + EPS) * gain + bias + left_rows[r]
            base[r * per_row + jh] = jnp.transpose(value)
    for u in range(2):
        for g in range(4):
            whole = tri_proj_ref[u, :, g * depth : (g + 1) * depth].astype(F32)
            weights[u, g] = jnp.transpose(whole).astype(BF16)
        gate_weights[u] = jnp.transpose(tri_gate_ref[u].astype(F32)).astype(BF16)
        out_weights[u] = jnp.transpose(tri_out_ref[u].astype(F32)).astype(BF16)
        columns[u, 0] = column(tri_gain_ref[u : u + 1, :])
        columns[u, 1] = column(tri_gate_bias_ref[u : u + 1, :])
        columns[u, 2] = column(tri_out_gain_ref[u : u + 1, :])
    size = rings * blocks
    perm[...] = selection((size, size), lambda q: lax.rem(q, blocks) * rings + q // blocks)
    perm_back[...] = selection((size, size), lambda q: lax.rem(q, rings) * blocks + q // rings)
    for half in range(2):
        pick[half] = selection((size, size), lambda q: q - lax.rem(q, 2) + half)
        pick_right[half] = selection(
            (size, 2 * size),
            lambda j: lax.rem(j // rows, 2) * size
            + (j // (2 * rows)) * blocks
            + 2 * lax.rem(j, rows)
            + half,
        )
    pick_left[...] = selection(
        (size, cols), lambda q: (q // blocks) * 2 * rows + rows * h + lax.rem(q, blocks) // 2
    )

    pl.semaphore_wait(barrier, rings - 1 + 1 + lanes_x - 1)

    def all_send(source, target, send, recv):
        def step(t, carry):
            peer = z_peer(t)
            pltpu.make_async_remote_copy(
                src_ref=source(peer),
                dst_ref=target(z),
                send_sem=send.at[peer],
                recv_sem=recv.at[z],
                device_id=to_z(peer),
                device_id_type=MESH,
            ).start()
            return carry

        lax.fori_loop(0, rings - 1, step, 0)

    def all_wait(source, target, send, recv, sent):
        def step(t, carry):
            peer = z_peer(rings - 2 - t)
            copy = pltpu.make_async_remote_copy(
                src_ref=source(peer),
                dst_ref=target(peer),
                send_sem=send.at[peer],
                recv_sem=recv.at[peer],
                device_id=to_z(peer),
                device_id_type=MESH,
            )
            if sent:
                copy.wait_send()
            else:
                copy.wait_recv()
            return carry

        lax.fori_loop(0, rings - 1, step, 0)

    def swap(buffer, k):
        def copy(parity):
            return pltpu.make_async_remote_copy(
                src_ref=buffer.at[parity],
                dst_ref=buffer.at[parity],
                send_sem=twin_send.at[k],
                recv_sem=twin_recv.at[k],
                device_id=twin,
                device_id_type=MESH,
            )

        copy(h).start()
        return copy(h), copy(1 - h)

    closing = []

    own_terms = lambda peer: terms.at[h, z]
    their_terms = lambda peer: terms.at[h, peer]
    all_send(own_terms, their_terms, terms_send, terms_recv)
    all_wait(own_terms, their_terms, terms_send, terms_recv, False)
    closing.append(functools.partial(all_wait, own_terms, their_terms, terms_send, terms_recv, True))
    sent, got = swap(terms, 0)
    got.wait_recv()
    closing.append(sent.wait_send)
    first, second = terms[0], terms[1]
    upper = lax.broadcasted_iota(jnp.int32, first.shape, 1) < rows
    right_whole = jnp.where(upper, first, second).reshape(cols, depth)
    mask_whole = jnp.where(upper, second, first)
    mask_whole = pltpu.roll(mask_whole, rows, 1).reshape(cols, depth)
    masks = []
    for jh in range(per_row):
        right_t = jnp.transpose(right_whole[jh * LANES : (jh + 1) * LANES])
        masks.append(jnp.transpose(mask_whole[jh * LANES : (jh + 1) * LANES])[:1])
        for r in range(rows):
            m = r * per_row + jh
            pair[m] = (base[m] + right_t).astype(BF16).astype(F32)

    for u in range(2):
        local = [
            weights[u, g, pl.ds(pl.multiple_of(x * width, width), width), :] for g in range(4)
        ]
        local = jnp.concatenate(local, axis=0)
        left_parts, right_parts = [], []
        for m in range(blocks):
            block = (norm_rows(pair[m]) * columns[u, 0]).astype(BF16)
            normed[m] = block
            projected = nn(local, block)
            masked = masks[m % per_row] * mask_of[m // per_row]
            value, gate = projected[:width], projected[width : 2 * width]
            left_parts.append((masked * jax.nn.sigmoid(gate) * value).astype(BF16))
            value, gate = projected[2 * width : 3 * width], projected[3 * width :]
            right_parts.append((masked * jax.nn.sigmoid(gate) * value).astype(BF16))
        for side, parts in enumerate((left_parts, right_parts)):
            ordered = nn(perm[...], jnp.concatenate(parts, axis=0)).astype(BF16)
            edges_out[u, side] = ordered.reshape(rings, blocks, LANES)

        for side, buffer in enumerate((left_in.at[u], right_in.at[u])):
            own = lambda peer, side=side: edges_out.at[u, side, peer]
            their = lambda peer, buffer=buffer: buffer.at[h, peer]
            all_send(own, their, edge_send.at[u, side], edge_recv.at[u, side])
            buffer[h, z] = edges_out[u, side, z]
        swaps = []
        for side, buffer in reversed(list(enumerate((left_in.at[u], right_in.at[u])))):
            own = lambda peer, side=side: edges_out.at[u, side, peer]
            their = lambda peer, buffer=buffer: buffer.at[h, peer]
            all_wait(own, their, edge_send.at[u, side], edge_recv.at[u, side], False)
            closing.append(
                functools.partial(
                    all_wait, own, their, edge_send.at[u, side], edge_recv.at[u, side], True
                )
            )
            if side == 1 or u == 1:
                swaps.append(swap(buffer, 1 + 2 * u + side))
        for sent, got in swaps:
            got.wait_recv()
            closing.append(sent.wait_send)

        right_rows_all = right_in[u].reshape(2 * size, LANES)
        if u == 0:
            left_own = left_in[u, h].reshape(size, LANES)
            a = [nn(pick[half], left_own).astype(BF16) for half in range(2)]
            b = [nn(pick_right[half], right_rows_all).astype(BF16) for half in range(2)]
            whole = nt(jnp.concatenate(a, axis=1), jnp.concatenate(b, axis=1))
            even = lax.rem(lax.broadcasted_iota(jnp.int32, (size, LANES), 0), 2) == 0
            product = jnp.where(even, whole[:, :LANES], whole[:, LANES:])
        else:
            spread = []
            for parity in range(2):
                block = left_in[u, parity].reshape(size, LANES)
                halves = [nn(pick[half], block).astype(BF16) for half in range(2)]
                spread.append(jnp.concatenate(halves, axis=1))
            chosen = nt(pick_left[...], jnp.concatenate(spread, axis=0))
            row_half = lax.rem(lax.broadcasted_iota(jnp.int32, chosen.shape, 0), 2)
            column_half = lax.rem(lax.broadcasted_iota(jnp.int32, chosen.shape, 1), 2)
            chosen = jnp.where(row_half == column_half, chosen, 0.0).astype(BF16)
            product = nn(chosen, right_rows_all)
        product_out[u] = product.astype(BF16).reshape(rings, blocks, LANES)

        own = lambda peer: product_out.at[u, peer]
        their = lambda peer: product_in.at[u, x, peer]
        all_send(own, their, back_send.at[u], back_recv.at[u])
        product_in[u, x, z] = product_out[u, z]
        all_wait(own, their, back_send.at[u], back_recv.at[u], False)
        closing.append(functools.partial(all_wait, own, their, back_send.at[u], back_recv.at[u], True))

        def lane_copy(t, source):
            return pltpu.make_async_remote_copy(
                src_ref=product_in.at[u, source],
                dst_ref=product_in.at[u, source],
                send_sem=lane_send.at[u, t],
                recv_sem=lane_recv.at[u, source],
                device_id={"chan": to_x(t)},
                device_id_type=MESH,
            )

        for t in (2, 1, 3) if lanes_x == 4 else range(1, lanes_x):
            lane_copy(t, x).start()
        gating = [
            jax.nn.sigmoid(nn(gate_weights[u], normed[m]) + columns[u, 1]) for m in range(blocks)
        ]
        for t in range(1, lanes_x):
            lane_copy(t, to_x(t)).wait_recv()
            closing.append(lane_copy(t, x).wait_send)
        hidden = [
            nn(perm_back[...], product_in[u, lane].reshape(size, LANES)) for lane in range(lanes_x)
        ]
        for m in range(blocks):
            block = jnp.concatenate([part[m * rings : (m + 1) * rings] for part in hidden], axis=0)
            block = (norm_rows(block) * columns[u, 2]).astype(BF16)
            update = nn(out_weights[u], block)
            value = pair[m] + gating[m] * update
            if u == 0:
                pair[m] = value.astype(BF16).astype(F32)
            else:
                r, jh = m // per_row, m % per_row
                out_ref[r, jh * LANES : (jh + 1) * LANES, :] = jnp.transpose(value).astype(BF16)

    for wait in closing:
        wait()


def body(
    prior_pair,
    single,
    target,
    residue_mask,
    recycle_gain,
    recycle_bias,
    left_single,
    right_single,
    left_target,
    right_target,
    tri_gain,
    tri_proj,
    tri_gate,
    tri_gate_bias,
    tri_out_gain,
    tri_out,
):
    rings = lax.axis_size("dap") // 2
    lanes_x = lax.axis_size("chan")
    rows, cols, depth = prior_pair.shape
    blocks = rows * cols // LANES
    size = rings * blocks
    vmem = pl.BlockSpec(memory_space=pltpu.VMEM)
    smem = pl.BlockSpec(memory_space=pltpu.SMEM)
    dma = pltpu.SemaphoreType.DMA
    return pl.pallas_call(
        functools.partial(kernel, rings, lanes_x),
        out_shape=jax.ShapeDtypeStruct(prior_pair.shape, BF16),
        in_specs=[vmem, vmem, smem, smem] + [vmem] * 12,
        out_specs=vmem,
        scratch_shapes=[
            pltpu.VMEM((2, rings, 2 * rows, LANES), F32),
            pltpu.VMEM((2, 2, rings, blocks, LANES), BF16),
            pltpu.VMEM((2, 2, rings, blocks, LANES), BF16),
            pltpu.VMEM((2, 2, rings, blocks, LANES), BF16),
            pltpu.VMEM((2, rings, blocks, LANES), BF16),
            pltpu.VMEM((2, lanes_x, rings, blocks, LANES), BF16),
            pltpu.VMEM((blocks, depth, LANES), F32),
            pltpu.VMEM((blocks, depth, LANES), F32),
            pltpu.VMEM((blocks, depth, LANES), BF16),
            pltpu.VMEM((2, 4, depth, depth), BF16),
            pltpu.VMEM((2, depth, depth), BF16),
            pltpu.VMEM((2, depth, depth), BF16),
            pltpu.VMEM((2, 3, depth, LANES), F32),
            pltpu.VMEM((size, size), BF16),
            pltpu.VMEM((size, size), BF16),
            pltpu.VMEM((2, size, size), BF16),
            pltpu.VMEM((2, size, 2 * size), BF16),
            pltpu.VMEM((size, cols), BF16),
            dma((rings,)),
            dma((rings,)),
            dma((2, 2, rings)),
            dma((2, 2, rings)),
            dma((2, rings)),
            dma((2, rings)),
            dma((5,)),
            dma((5,)),
            dma((2, lanes_x)),
            dma((2, lanes_x)),
        ],
        compiler_params=pltpu.CompilerParams(collective_id=0, has_side_effects=True),
        name="triangles",
    )(
        prior_pair,
        single,
        target,
        residue_mask,
        recycle_gain[None, :],
        recycle_bias[None, :],
        left_single,
        right_single,
        left_target,
        right_target,
        tri_gain,
        tri_proj.reshape(2, depth, -1),
        tri_gate,
        tri_gate_bias,
        tri_out_gain,
        tri_out,
    )


def solution(mesh):
    rows = P(("crops", "dap"))
    placed = (P(("crops", "dap"), None, None), P(("crops", "dap"), None), rows, rows) + (P(),) * 12
    return jax.shard_map(
        body, mesh=mesh, in_specs=placed, out_specs=P(("crops", "dap"), None, None), check_vma=False
    )
```

```python
import functools

import jax
import jax.numpy as jnp
from jax import lax
from jax.experimental import pallas as pl
from jax.experimental.pallas import tpu as pltpu
from jax.sharding import PartitionSpec as P

F32 = jnp.float32
BF16 = jnp.bfloat16
MESH = pl.DeviceIdType.MESH
EPS = 1e-05
LANES = 128
GROUP = 8


def selection(shape, column_of_row):
    rows = lax.broadcasted_iota(jnp.int32, shape, 0)
    columns = lax.broadcasted_iota(jnp.int32, shape, 1)
    return jnp.where(columns == column_of_row(rows), 1.0, 0.0).astype(BF16)


def nn(a, b):
    return lax.dot_general(a, b, (((1,), (0,)), ((), ())), preferred_element_type=F32)


def nt(a, b):
    return lax.dot_general(a, b, (((1,), (1,)), ((), ())), preferred_element_type=F32)


def norm_rows(values):
    scale = 1.0 / values.shape[0]
    center = values - jnp.sum(values, axis=0, keepdims=True) * scale
    spread = jnp.sum(center * center, axis=0, keepdims=True) * scale
    return center * lax.rsqrt(spread + EPS)


class Phases:
    def __init__(self):
        self.scope = None

    def __call__(self, name):
        if self.scope is not None:
            self.scope.__exit__(None, None, None)
        self.scope = jax.named_scope(name) if name else None
        if self.scope is not None:
            self.scope.__enter__()


def column(row_vector):
    return jnp.transpose(jnp.broadcast_to(row_vector, (LANES, LANES)))


def kernel(
    rings,
    lanes_x,
    prior_hbm,
    single_hbm,
    target_hbm,
    mask_hbm,
    recycle_gain_hbm,
    recycle_bias_hbm,
    left_single_hbm,
    right_single_hbm,
    left_target_hbm,
    right_target_hbm,
    tri_gain_hbm,
    tri_proj_hbm,
    tri_gate_hbm,
    tri_gate_bias_hbm,
    tri_out_gain_hbm,
    tri_out_hbm,
    out_ref,
    prior_ref,
    single_ref,
    target_ref,
    mask_ref,
    recycle_gain_ref,
    recycle_bias_ref,
    left_single_ref,
    right_single_ref,
    left_target_ref,
    right_target_ref,
    tri_gain_ref,
    tri_proj_ref,
    tri_gate_ref,
    tri_gate_bias_ref,
    tri_out_gain_ref,
    tri_out_ref,
    terms,
    edges_out,
    edges_in,
    product_out,
    product_in,
    base,
    pair,
    normed,
    weights,
    gate_weights,
    out_weights,
    columns,
    perm,
    perm_back,
    pick,
    pick_right,
    pick_left,
    load_sem,
    terms_sem,
    edge_sem,
    back_send,
    back_recv,
    twin_send,
    twin_recv,
    lane_sem,
):
    rows, cols, depth = prior_ref.shape
    blocks = rows * cols // LANES
    per_row = cols // LANES
    width = depth // lanes_x
    size = rings * blocks
    dap = lax.axis_index("dap")
    x = lax.axis_index("chan")
    z = dap // 2
    h = lax.rem(dap, 2)
    twin = {"dap": dap + 1 - 2 * h}
    phase = Phases()

    def offset(p):
        up = (p + 1) // 2
        return rings + up * (2 * lax.rem(p, 2) - 1)

    def to_z(peer):
        return {"dap": 2 * peer + h}

    def to_x(t):
        return lax.rem(x + t, lanes_x)

    phase("greet")
    barrier = pltpu.get_barrier_semaphore()

    def greet(t, carry):
        peer = lax.rem(z + offset(rings - 1 - t), rings)
        pl.semaphore_signal(barrier, inc=1, device_id=to_z(peer), device_id_type=MESH)
        return carry

    lax.fori_loop(0, rings - 1, greet, 0)
    pl.semaphore_signal(barrier, inc=1, device_id=twin, device_id_type=MESH)
    for t in range(1, lanes_x):
        pl.semaphore_signal(barrier, inc=1, device_id={"chan": to_x(t)}, device_id_type=MESH)

    loads = {}
    sources = (
        (single_hbm, single_ref),
        (right_single_hbm, right_single_ref),
        (target_hbm, target_ref),
        (mask_hbm, mask_ref),
        (right_target_hbm, right_target_ref),
        (left_single_hbm, left_single_ref),
        (left_target_hbm, left_target_ref),
        (recycle_gain_hbm, recycle_gain_ref),
        (recycle_bias_hbm, recycle_bias_ref),
        (prior_hbm, prior_ref),
        (tri_proj_hbm, tri_proj_ref),
        (tri_gain_hbm, tri_gain_ref),
        (tri_gate_hbm, tri_gate_ref),
        (tri_gate_bias_hbm, tri_gate_bias_ref),
        (tri_out_gain_hbm, tri_out_gain_ref),
        (tri_out_hbm, tri_out_ref),
    )
    loads = [
        pltpu.make_async_copy(source, held, load_sem.at[n])
        for n, (source, held) in enumerate(sources)
    ]
    for load in loads:
        load.start()

    phase("terms")
    for load in loads[:5]:
        load.wait()
    single = single_ref[...]
    mask_of = [mask_ref[r].astype(F32) for r in range(rows)]

    def row_terms(weight_ref, table_ref):
        linear = nn(single, weight_ref[...])
        table = table_ref[...].astype(F32)
        classes = lax.broadcasted_iota(jnp.int32, table.shape, 0)
        picked = [
            jnp.sum(jnp.where(classes == target_ref[r], table, 0.0), axis=0, keepdims=True)
            for r in range(rows)
        ]
        return [linear[r : r + 1] + picked[r] for r in range(rows)]

    right_rows = row_terms(right_single_ref, right_target_ref)
    mask_rows = [jnp.full((1, depth), mask_of[r], F32) for r in range(rows)]
    tile = jnp.concatenate(right_rows + mask_rows, axis=0)
    terms[h, z] = jnp.where(h == 0, tile, pltpu.roll(tile, rows, 0))

    phase("barrier")
    pl.semaphore_wait(barrier, rings - 1 + 1 + lanes_x - 1)

    def remote(source, target, send, recv, device):
        return pltpu.make_async_remote_copy(
            src_ref=source,
            dst_ref=target,
            send_sem=send,
            recv_sem=recv,
            device_id=device,
            device_id_type=MESH,
        )

    closing = []

    phase("tsend")

    def send_terms(t, carry):
        peer = lax.rem(z + offset(rings - 1 - t), rings)
        remote(terms.at[h, z], terms.at[h, z], terms_sem.at[0], terms_sem.at[1], to_z(peer)).start()
        return carry

    lax.fori_loop(0, rings - 1, send_terms, 0)
    many = terms.at[h, pl.ds(0, rings - 1)]
    terms_all = remote(many, many, terms_sem.at[0], terms_sem.at[1], twin)
    closing.append(terms_all.wait_send)

    phase("local")
    for load in loads[5:]:
        load.wait()
    left_rows = row_terms(left_single_ref, left_target_ref)
    gain = recycle_gain_ref[...]
    bias = recycle_bias_ref[...]
    for r in range(rows):
        for jh in range(per_row):
            block = prior_ref[r, jh * LANES : (jh + 1) * LANES, :].astype(F32)
            center = block - jnp.mean(block, axis=1, keepdims=True)
            spread = jnp.mean(center * center, axis=1, keepdims=True)
            value = center * lax.rsqrt(spread + EPS) * gain + bias + left_rows[r]
            base[r * per_row + jh] = jnp.transpose(value)
    for u in range(2):
        whole = tri_proj_ref[u].astype(F32)
        for g in range(4):
            weights[u, g] = jnp.transpose(whole[:, g, :]).astype(BF16)
        gate_weights[u] = jnp.transpose(tri_gate_ref[u].astype(F32)).astype(BF16)
        out_weights[u] = jnp.transpose(tri_out_ref[u].astype(F32)).astype(BF16)
        columns[u, 0] = column(tri_gain_ref[u : u + 1, :])
        columns[u, 1] = column(tri_gate_bias_ref[u : u + 1, :])
        columns[u, 2] = column(tri_out_gain_ref[u : u + 1, :])

    def place(channel):
        delta = lax.rem(channel - z + rings, rings)
        after = jnp.where(delta <= rings // 2, 2 * delta - 1, 2 * (rings - delta))
        return jnp.where(delta == 0, 0, after)

    perm[...] = selection((size, size), lambda q: lax.rem(q, blocks) * rings + q // blocks)
    perm_back[...] = selection(
        (size, size), lambda q: place(lax.rem(q, rings)) * blocks + q // rings
    )
    for half in range(2):
        pick[half] = selection((size, size), lambda q: q - lax.rem(q, 2) + half)
        pick_right[half] = selection(
            (size, 2 * size),
            lambda j: lax.rem(j // rows, 2) * size
            + (j // (2 * rows)) * blocks
            + 2 * lax.rem(j, rows)
            + half,
        )
    pick_left[...] = selection(
        (size, cols), lambda q: (q // blocks) * 2 * rows + rows * h + lax.rem(q, blocks) // 2
    )

    phase("twait")
    terms_all.wait_recv()
    phase("ttwin")

    def swap(view, k):
        def copy(parity):
            return remote(view(parity), view(parity), twin_send.at[k], twin_recv.at[k], twin)

        copy(h).start()
        closing.append(copy(h).wait_send)
        copy(1 - h).wait_recv()

    swap(lambda parity: terms.at[parity], 0)

    phase("pair")
    first, second = terms[0], terms[1]
    upper = lax.broadcasted_iota(jnp.int32, first.shape, 1) < rows
    right_whole = jnp.where(upper, first, second).reshape(cols, depth)
    mask_whole = jnp.where(upper, second, first)
    mask_whole = pltpu.roll(mask_whole, rows, 1).reshape(cols, depth)
    masks = []
    for jh in range(per_row):
        right_t = jnp.transpose(right_whole[jh * LANES : (jh + 1) * LANES])
        masks.append(jnp.transpose(mask_whole[jh * LANES : (jh + 1) * LANES])[:1])
        for r in range(rows):
            m = r * per_row + jh
            pair[m] = (base[m] + right_t).astype(BF16).astype(F32)

    for u in range(2):
        phase("edges")
        local = [
            weights[u, g, pl.ds(pl.multiple_of(x * width, width), width), :] for g in range(4)
        ]
        local = jnp.concatenate(local, axis=0)
        left_parts, right_parts = [], []
        for m in range(blocks):
            block = (norm_rows(pair[m]) * columns[u, 0]).astype(BF16)
            normed[m] = block
            projected = nn(local, block)
            masked = masks[m % per_row] * mask_of[m // per_row]
            value, gate = projected[:width], projected[width : 2 * width]
            left_parts.append((masked * jax.nn.sigmoid(gate) * value).astype(BF16))
            value, gate = projected[2 * width : 3 * width], projected[3 * width :]
            right_parts.append((masked * jax.nn.sigmoid(gate) * value).astype(BF16))
        for side, parts in enumerate((left_parts, right_parts)):
            ordered = nn(perm[...], jnp.concatenate(parts, axis=0)).astype(BF16)
            edges_out[u, :, side] = ordered.reshape(rings, blocks, LANES)

        phase("esend")

        def send_edges(t, carry, u=u):
            peer = lax.rem(z + offset(rings - 1 - t), rings)
            remote(
                edges_out.at[u, peer],
                edges_in.at[u, h, z],
                edge_sem.at[u, 0],
                edge_sem.at[u, 1],
                to_z(peer),
            ).start()
            return carry

        lax.fori_loop(0, rings - 1, send_edges, 0)
        edges_in[u, h, z] = edges_out[u, z]
        gating = [
            jax.nn.sigmoid(nn(gate_weights[u], normed[m]) + columns[u, 1]) for m in range(blocks)
        ]
        many = edges_in.at[u, h, pl.ds(0, rings - 1)]
        edges_all = remote(many, many, edge_sem.at[u, 0], edge_sem.at[u, 1], twin)
        closing.append(edges_all.wait_send)
        phase("ewait")
        edges_all.wait_recv()
        phase("etwin")
        if u == 0:
            swap(lambda parity: edges_in.at[0, parity, :, 1], 1)
        else:
            swap(lambda parity: edges_in.at[1, parity], 2)

        phase("product")
        right_rows_all = edges_in[u, :, :, 1].reshape(2 * size, LANES)
        if u == 0:
            left_own = edges_in[u, h, :, 0].reshape(size, LANES)
            a = [nn(pick[half], left_own).astype(BF16) for half in range(2)]
            b = [nn(pick_right[half], right_rows_all).astype(BF16) for half in range(2)]
            whole = nt(jnp.concatenate(a, axis=1), jnp.concatenate(b, axis=1))
            even = lax.rem(lax.broadcasted_iota(jnp.int32, (size, LANES), 0), 2) == 0
            product = jnp.where(even, whole[:, :LANES], whole[:, LANES:])
        else:
            spread = []
            for parity in range(2):
                block = edges_in[u, parity, :, 0].reshape(size, LANES)
                halves = [nn(pick[half], block).astype(BF16) for half in range(2)]
                spread.append(jnp.concatenate(halves, axis=1))
            chosen = nt(pick_left[...], jnp.concatenate(spread, axis=0))
            row_half = lax.rem(lax.broadcasted_iota(jnp.int32, chosen.shape, 0), 2)
            column_half = lax.rem(lax.broadcasted_iota(jnp.int32, chosen.shape, 1), 2)
            chosen = jnp.where(row_half == column_half, chosen, 0.0).astype(BF16)
            product = nn(chosen, right_rows_all)
        product_out[u] = product.astype(BF16).reshape(rings, blocks, LANES)

        phase("bsend")

        def send_back(t, carry, u=u):
            p = rings - 1 - t
            peer = lax.rem(z + 2 * rings - offset(p), rings)
            remote(
                product_out.at[u, peer],
                product_in.at[u, x, p],
                back_send.at[u],
                back_recv.at[u, (p - 1) // GROUP],
                to_z(peer),
            ).start()
            return carry

        lax.fori_loop(0, rings - 1, send_back, 0)
        product_in[u, x, 0] = product_out[u, z]
        many = product_out.at[u, pl.ds(0, rings - 1)]
        closing.append(remote(many, many, back_send.at[u], back_recv.at[u, 0], twin).wait_send)
        phase("bwait")
        for g, start in enumerate(range(1, rings, GROUP)):
            arrived = product_in.at[u, x, pl.ds(start, min(GROUP, rings - start))]
            remote(arrived, arrived, back_send.at[u], back_recv.at[u, g], twin).wait_recv()
            begin = start if g else 0
            part = product_in.at[u, x, pl.ds(begin, min(start + GROUP, rings) - begin)]
            for t in (2, 1, 3) if lanes_x == 4 else range(1, lanes_x):
                remote(part, part, lane_sem.at[u, 0], lane_sem.at[u, 1], {"chan": to_x(t)}).start()
        phase("lwait")
        many = product_in.at[u, pl.ds(0, lanes_x - 1)]
        lanes_all = remote(many, many, lane_sem.at[u, 0], lane_sem.at[u, 1], twin)
        lanes_all.wait_recv()
        closing.append(lanes_all.wait_send)

        phase("hidden")
        hidden = [
            nn(perm_back[...], product_in[u, lane].reshape(size, LANES)) for lane in range(lanes_x)
        ]
        for m in range(blocks):
            block = jnp.concatenate([part[m * rings : (m + 1) * rings] for part in hidden], axis=0)
            block = (norm_rows(block) * columns[u, 2]).astype(BF16)
            update = nn(out_weights[u], block)
            value = pair[m] + gating[m] * update
            if u == 0:
                pair[m] = value.astype(BF16).astype(F32)
            else:
                r, jh = m // per_row, m % per_row
                out_ref[r, jh * LANES : (jh + 1) * LANES, :] = jnp.transpose(value).astype(BF16)

    phase("close")
    for wait in closing:
        wait()
    phase(None)


def body(
    prior_pair,
    single,
    target,
    residue_mask,
    recycle_gain,
    recycle_bias,
    left_single,
    right_single,
    left_target,
    right_target,
    tri_gain,
    tri_proj,
    tri_gate,
    tri_gate_bias,
    tri_out_gain,
    tri_out,
):
    rings = lax.axis_size("dap") // 2
    lanes_x = lax.axis_size("chan")
    rows, cols, depth = prior_pair.shape
    blocks = rows * cols // LANES
    size = rings * blocks
    groups = -(-(rings - 1) // GROUP)
    vmem = pl.BlockSpec(memory_space=pltpu.VMEM)
    hbm = pl.BlockSpec(memory_space=pltpu.HBM)
    dma = pltpu.SemaphoreType.DMA
    operands = (
        prior_pair,
        single,
        target,
        residue_mask,
        recycle_gain[None, :],
        recycle_bias[None, :],
        left_single,
        right_single,
        left_target,
        right_target,
        tri_gain,
        tri_proj,
        tri_gate,
        tri_gate_bias,
        tri_out_gain,
        tri_out,
    )
    held = [
        pltpu.SMEM(a.shape, a.dtype) if a.dtype == jnp.int32 else pltpu.VMEM(a.shape, a.dtype)
        for a in operands
    ]
    return pl.pallas_call(
        functools.partial(kernel, rings, lanes_x),
        out_shape=jax.ShapeDtypeStruct(prior_pair.shape, BF16),
        in_specs=[hbm] * len(operands),
        out_specs=vmem,
        scratch_shapes=held
        + [
            pltpu.VMEM((2, rings, 2 * rows, LANES), F32),
            pltpu.VMEM((2, rings, 2, blocks, LANES), BF16),
            pltpu.VMEM((2, 2, rings, 2, blocks, LANES), BF16),
            pltpu.VMEM((2, rings, blocks, LANES), BF16),
            pltpu.VMEM((2, lanes_x, rings, blocks, LANES), BF16),
            pltpu.VMEM((blocks, depth, LANES), F32),
            pltpu.VMEM((blocks, depth, LANES), F32),
            pltpu.VMEM((blocks, depth, LANES), BF16),
            pltpu.VMEM((2, 4, depth, depth), BF16),
            pltpu.VMEM((2, depth, depth), BF16),
            pltpu.VMEM((2, depth, depth), BF16),
            pltpu.VMEM((2, 3, depth, LANES), F32),
            pltpu.VMEM((size, size), BF16),
            pltpu.VMEM((size, size), BF16),
            pltpu.VMEM((2, size, size), BF16),
            pltpu.VMEM((2, size, 2 * size), BF16),
            pltpu.VMEM((size, cols), BF16),
            dma((len(operands),)),
            dma((2,)),
            dma((2, 2)),
            dma((2,)),
            dma((2, groups)),
            dma((3,)),
            dma((3,)),
            dma((2, 2)),
        ],
        compiler_params=pltpu.CompilerParams(collective_id=0, has_side_effects=True),
        name="triangles",
    )(*operands)


def solution(mesh):
    rows = P(("crops", "dap"))
    placed = (P(("crops", "dap"), None, None), P(("crops", "dap"), None), rows, rows) + (P(),) * 12
    return jax.shard_map(
        body, mesh=mesh, in_specs=placed, out_specs=P(("crops", "dap"), None, None), check_vma=False
    )
```

```python
import functools

import jax
import jax.numpy as jnp
from jax import lax
from jax.experimental import pallas as pl
from jax.experimental.pallas import tpu as pltpu
from jax.sharding import PartitionSpec as P

F32 = jnp.float32
BF16 = jnp.bfloat16
MESH = pl.DeviceIdType.MESH
EPS = 1e-05
LANES = 128
GROUP = 8
STRIDE = 4


def selection(shape, column_of_row):
    rows = lax.broadcasted_iota(jnp.int32, shape, 0)
    columns = lax.broadcasted_iota(jnp.int32, shape, 1)
    return jnp.where(columns == column_of_row(rows), 1.0, 0.0).astype(BF16)


def nn(a, b):
    return lax.dot_general(a, b, (((1,), (0,)), ((), ())), preferred_element_type=F32)


def nt(a, b):
    return lax.dot_general(a, b, (((1,), (1,)), ((), ())), preferred_element_type=F32)


def norm_rows(values):
    scale = 1.0 / values.shape[0]
    center = values - jnp.sum(values, axis=0, keepdims=True) * scale
    spread = jnp.sum(center * center, axis=0, keepdims=True) * scale
    return center * lax.rsqrt(spread + EPS)


class Phases:
    def __init__(self):
        self.scope = None

    def __call__(self, name):
        if self.scope is not None:
            self.scope.__exit__(None, None, None)
        self.scope = jax.named_scope(name) if name else None
        if self.scope is not None:
            self.scope.__enter__()


def column(row_vector):
    return jnp.transpose(jnp.broadcast_to(row_vector, (LANES, LANES)))


def kernel(
    rings,
    lanes_x,
    prior_hbm,
    single_hbm,
    target_hbm,
    mask_hbm,
    recycle_gain_hbm,
    recycle_bias_hbm,
    left_single_hbm,
    right_single_hbm,
    left_target_hbm,
    right_target_hbm,
    tri_gain_hbm,
    tri_proj_hbm,
    tri_gate_hbm,
    tri_gate_bias_hbm,
    tri_out_gain_hbm,
    tri_out_hbm,
    out_ref,
    prior_ref,
    single_ref,
    target_ref,
    mask_ref,
    recycle_gain_ref,
    recycle_bias_ref,
    left_single_ref,
    right_single_ref,
    left_target_ref,
    right_target_ref,
    tri_gain_ref,
    tri_proj_ref,
    tri_gate_ref,
    tri_gate_bias_ref,
    tri_out_gain_ref,
    tri_out_ref,
    terms,
    edges_out,
    edges_in,
    product_out,
    product_in,
    base,
    pair,
    normed,
    weights,
    gate_weights,
    out_weights,
    columns,
    perm,
    perm_back,
    pick,
    pick_right,
    pick_left,
    load_sem,
    terms_send,
    terms_recv,
    edge_sem,
    back_send,
    back_recv,
    twin_send,
    twin_recv,
    lane_sem,
):
    rows, cols, depth = prior_ref.shape
    blocks = rows * cols // LANES
    per_row = cols // LANES
    width = depth // lanes_x
    size = rings * blocks
    dap = lax.axis_index("dap")
    x = lax.axis_index("chan")
    z = dap // 2
    h = lax.rem(dap, 2)
    twin = {"dap": dap + 1 - 2 * h}
    phase = Phases()

    def offset(p):
        up = (p + 1) // 2
        return rings + up * (2 * lax.rem(p, 2) - 1)

    def to_z(peer):
        return {"dap": 2 * peer + h}

    def to_x(t):
        return lax.rem(x + t, lanes_x)

    phase("greet")
    barrier = pltpu.get_barrier_semaphore()

    q = lax.rem(z + rings - 1, rings)
    last = rings - 1

    def at(order):
        return to_z(lax.rem(order + 1, rings))

    def greet(order):
        pl.semaphore_signal(barrier, inc=1, device_id=at(order), device_id_type=MESH)

    for back in range(1, STRIDE + 1):
        pl.when(q >= back)(functools.partial(greet, q - back))
    pl.semaphore_signal(barrier, inc=1, device_id=twin, device_id_type=MESH)
    for t in range(1, lanes_x):
        pl.semaphore_signal(barrier, inc=1, device_id={"chan": to_x(t)}, device_id_type=MESH)

    sources = (
        (single_hbm, single_ref),
        (right_single_hbm, right_single_ref),
        (target_hbm, target_ref),
        (mask_hbm, mask_ref),
        (right_target_hbm, right_target_ref),
        (left_single_hbm, left_single_ref),
        (left_target_hbm, left_target_ref),
        (recycle_gain_hbm, recycle_gain_ref),
        (recycle_bias_hbm, recycle_bias_ref),
        (prior_hbm, prior_ref),
        (tri_proj_hbm, tri_proj_ref),
        (tri_gain_hbm, tri_gain_ref),
        (tri_gate_hbm, tri_gate_ref),
        (tri_gate_bias_hbm, tri_gate_bias_ref),
        (tri_out_gain_hbm, tri_out_gain_ref),
        (tri_out_hbm, tri_out_ref),
    )
    loads = [
        pltpu.make_async_copy(source, held, load_sem.at[n])
        for n, (source, held) in enumerate(sources)
    ]
    for load in loads:
        load.start()

    def greet_later(order, carry):
        greet(order)
        return carry

    lax.fori_loop(q + 1, rings, greet_later, 0)

    phase("terms")
    for load in loads[:5]:
        load.wait()
    single = single_ref[...]
    mask_of = [mask_ref[r].astype(F32) for r in range(rows)]

    def row_terms(weight_ref, table_ref):
        linear = nn(single, weight_ref[...])
        table = table_ref[...].astype(F32)
        classes = lax.broadcasted_iota(jnp.int32, table.shape, 0)
        picked = [
            jnp.sum(jnp.where(classes == target_ref[r], table, 0.0), axis=0, keepdims=True)
            for r in range(rows)
        ]
        return [linear[r : r + 1] + picked[r] for r in range(rows)]

    right_rows = row_terms(right_single_ref, right_target_ref)
    mask_rows = [jnp.full((1, depth), mask_of[r], F32) for r in range(rows)]
    tile = jnp.concatenate(right_rows + mask_rows, axis=0)
    terms[h, z] = jnp.where(h == 0, tile, pltpu.roll(tile, rows, 0))

    phase("barrier")
    pl.semaphore_wait(barrier, q + jnp.minimum(STRIDE, last - q) + 1 + lanes_x - 1)

    def remote(source, target, send, recv, device):
        return pltpu.make_async_remote_copy(
            src_ref=source,
            dst_ref=target,
            send_sem=send,
            recv_sem=recv,
            device_id=device,
            device_id_type=MESH,
        )

    closing = []

    phase("tsend")

    def give(source, order):
        tile = terms.at[h, source]
        remote(tile, tile, terms_send.at[0], terms_recv.at[source], at(order)).start()

    def carried(source):
        return lax.rem(source, lanes_x) == x

    for ahead in range(1, STRIDE + 1):
        pl.when(carried(z) & (q + ahead <= last))(functools.partial(give, z, q + ahead))

    def give_earlier(t, carry):
        order = lax.rem(q + offset(rings - 1 - t), rings)
        pl.when(order < q)(functools.partial(give, z, order))
        return carry

    lax.fori_loop(0, rings - 1, give_earlier, 0)

    def await_terms(source):
        tile = terms.at[h, source]
        remote(tile, tile, terms_send.at[0], terms_recv.at[source], twin).wait_recv()

    early = q + STRIDE <= last

    def lower(order):
        return lax.rem(order + 1, rings)

    def hand_over(source):
        tile = terms.at[h, source]
        for lane in range(1, lanes_x):
            to = {"chan": to_x(lane)}
            remote(tile, tile, terms_send.at[0], terms_recv.at[source], to).start()

    def relay(order, carry):
        source = lower(order)

        @pl.when(carried(source))
        def _():
            await_terms(source)
            pl.when(early)(functools.partial(give, source, q + STRIDE))
            pl.when(jnp.logical_not(early))(functools.partial(hand_over, source))

        return carry

    def hand_over_all(order, carry):
        source = lower(order)
        pl.when(carried(source))(functools.partial(hand_over, source))
        return carry

    def relay_all():
        lax.fori_loop(0, q, relay, 0)
        lax.fori_loop(0, jnp.where(early, q, 0), hand_over_all, 0)

    def collect(order, carry):
        source = lower(order)
        pl.when(jnp.logical_not(carried(source)))(functools.partial(await_terms, source))
        return carry

    def prepare():
        for load in loads[5:]:
            load.wait()
        left_rows = row_terms(left_single_ref, left_target_ref)
        gain = recycle_gain_ref[...]
        bias = recycle_bias_ref[...]
        for r in range(rows):
            for jh in range(per_row):
                block = prior_ref[r, jh * LANES : (jh + 1) * LANES, :].astype(F32)
                center = block - jnp.mean(block, axis=1, keepdims=True)
                spread = jnp.mean(center * center, axis=1, keepdims=True)
                value = center * lax.rsqrt(spread + EPS) * gain + bias + left_rows[r]
                base[r * per_row + jh] = jnp.transpose(value)
        for u in range(2):
            whole = tri_proj_ref[u].astype(F32)
            for g in range(4):
                weights[u, g] = jnp.transpose(whole[:, g, :]).astype(BF16)
            gate_weights[u] = jnp.transpose(tri_gate_ref[u].astype(F32)).astype(BF16)
            out_weights[u] = jnp.transpose(tri_out_ref[u].astype(F32)).astype(BF16)
            columns[u, 0] = column(tri_gain_ref[u : u + 1, :])
            columns[u, 1] = column(tri_gate_bias_ref[u : u + 1, :])
            columns[u, 2] = column(tri_out_gain_ref[u : u + 1, :])

        def place(channel):
            delta = lax.rem(channel - z + rings, rings)
            after = jnp.where(delta <= rings // 2, 2 * delta - 1, 2 * (rings - delta))
            return jnp.where(delta == 0, 0, after)

        perm[...] = selection((size, size), lambda q: lax.rem(q, blocks) * rings + q // blocks)
        perm_back[...] = selection(
            (size, size), lambda q: place(lax.rem(q, rings)) * blocks + q // rings
        )
        for half in range(2):
            pick[half] = selection((size, size), lambda q: q - lax.rem(q, 2) + half)
            pick_right[half] = selection(
                (size, 2 * size),
                lambda j: lax.rem(j // rows, 2) * size
                + (j // (2 * rows)) * blocks
                + 2 * lax.rem(j, rows)
                + half,
            )
        pick_left[...] = selection(
            (size, cols), lambda q: (q // blocks) * 2 * rows + rows * h + lax.rem(q, blocks) // 2
        )

    phase("relay")

    def turn(step, carry):
        pl.when((step == 0) == early)(relay_all)
        pl.when((step == 1) == early)(prepare)
        return carry

    lax.fori_loop(0, 2, turn, 0)

    phase("twait")
    def later(order, carry):
        await_terms(lax.rem(order + 1, rings))
        return carry

    lax.fori_loop(0, q, collect, 0)
    lax.fori_loop(q + 1, rings, later, 0)
    phase("ttwin")

    def swap(view, k):
        def copy(parity):
            return remote(view(parity), view(parity), twin_send.at[k], twin_recv.at[k], twin)

        copy(h).start()
        closing.append(copy(h).wait_send)
        copy(1 - h).wait_recv()

    swap(lambda parity: terms.at[parity], 0)

    phase("pair")
    first, second = terms[0], terms[1]
    upper = lax.broadcasted_iota(jnp.int32, first.shape, 1) < rows
    right_whole = jnp.where(upper, first, second).reshape(cols, depth)
    mask_whole = jnp.where(upper, second, first)
    mask_whole = pltpu.roll(mask_whole, rows, 1).reshape(cols, depth)
    masks = []
    for jh in range(per_row):
        right_t = jnp.transpose(right_whole[jh * LANES : (jh + 1) * LANES])
        masks.append(jnp.transpose(mask_whole[jh * LANES : (jh + 1) * LANES])[:1])
        for r in range(rows):
            m = r * per_row + jh
            pair[m] = (base[m] + right_t).astype(BF16).astype(F32)

    for u in range(2):
        phase("edges")
        local = [
            weights[u, g, pl.ds(pl.multiple_of(x * width, width), width), :] for g in range(4)
        ]
        local = jnp.concatenate(local, axis=0)
        left_parts, right_parts = [], []
        for m in range(blocks):
            block = (norm_rows(pair[m]) * columns[u, 0]).astype(BF16)
            normed[m] = block
            projected = nn(local, block)
            masked = masks[m % per_row] * mask_of[m // per_row]
            value, gate = projected[:width], projected[width : 2 * width]
            left_parts.append((masked * jax.nn.sigmoid(gate) * value).astype(BF16))
            value, gate = projected[2 * width : 3 * width], projected[3 * width :]
            right_parts.append((masked * jax.nn.sigmoid(gate) * value).astype(BF16))
        for side, parts in enumerate((left_parts, right_parts)):
            ordered = nn(perm[...], jnp.concatenate(parts, axis=0)).astype(BF16)
            edges_out[u, :, side] = ordered.reshape(rings, blocks, LANES)

        phase("esend")

        def send_edges(t, carry, u=u):
            peer = lax.rem(z + offset(rings - 1 - t), rings)
            remote(
                edges_out.at[u, peer],
                edges_in.at[u, h, z],
                edge_sem.at[u, 0],
                edge_sem.at[u, 1],
                to_z(peer),
            ).start()
            return carry

        lax.fori_loop(0, rings - 1, send_edges, 0)
        edges_in[u, h, z] = edges_out[u, z]
        gating = [
            jax.nn.sigmoid(nn(gate_weights[u], normed[m]) + columns[u, 1]) for m in range(blocks)
        ]
        many = edges_in.at[u, h, pl.ds(0, rings - 1)]
        edges_all = remote(many, many, edge_sem.at[u, 0], edge_sem.at[u, 1], twin)
        closing.append(edges_all.wait_send)
        if u == 0:
            relayed = (q - x + lanes_x) // lanes_x - jnp.where(x == 0, 1, 0)
            copies = lanes_x - 1 + jnp.where(q + STRIDE <= last, 1, 0)
            ahead = jnp.where(carried(z), jnp.minimum(STRIDE, last - q), 0)
            given = ahead + q + relayed * copies

            def gone(t, carry):
                tile = terms.at[h, z]
                remote(tile, tile, terms_send.at[0], terms_recv.at[z], twin).wait_send()
                return carry

            lax.fori_loop(0, given, gone, 0)
        phase("ewait")
        edges_all.wait_recv()
        phase("etwin")
        if u == 0:
            swap(lambda parity: edges_in.at[0, parity, :, 1], 1)
        else:
            swap(lambda parity: edges_in.at[1, parity], 2)

        phase("product")
        right_rows_all = edges_in[u, :, :, 1].reshape(2 * size, LANES)
        if u == 0:
            left_own = edges_in[u, h, :, 0].reshape(size, LANES)
            a = [nn(pick[half], left_own).astype(BF16) for half in range(2)]
            b = [nn(pick_right[half], right_rows_all).astype(BF16) for half in range(2)]
            whole = nt(jnp.concatenate(a, axis=1), jnp.concatenate(b, axis=1))
            even = lax.rem(lax.broadcasted_iota(jnp.int32, (size, LANES), 0), 2) == 0
            product = jnp.where(even, whole[:, :LANES], whole[:, LANES:])
        else:
            spread = []
            for parity in range(2):
                block = edges_in[u, parity, :, 0].reshape(size, LANES)
                halves = [nn(pick[half], block).astype(BF16) for half in range(2)]
                spread.append(jnp.concatenate(halves, axis=1))
            chosen = nt(pick_left[...], jnp.concatenate(spread, axis=0))
            row_half = lax.rem(lax.broadcasted_iota(jnp.int32, chosen.shape, 0), 2)
            column_half = lax.rem(lax.broadcasted_iota(jnp.int32, chosen.shape, 1), 2)
            chosen = jnp.where(row_half == column_half, chosen, 0.0).astype(BF16)
            product = nn(chosen, right_rows_all)
        product_out[u] = product.astype(BF16).reshape(rings, blocks, LANES)

        phase("bsend")

        def send_back(t, carry, u=u):
            p = rings - 1 - t
            peer = lax.rem(z + 2 * rings - offset(p), rings)
            remote(
                product_out.at[u, peer],
                product_in.at[u, x, p],
                back_send.at[u],
                back_recv.at[u, (p - 1) // GROUP],
                to_z(peer),
            ).start()
            return carry

        lax.fori_loop(0, rings - 1, send_back, 0)
        product_in[u, x, 0] = product_out[u, z]
        many = product_out.at[u, pl.ds(0, rings - 1)]
        closing.append(remote(many, many, back_send.at[u], back_recv.at[u, 0], twin).wait_send)
        phase("bwait")
        for g, start in enumerate(range(1, rings, GROUP)):
            arrived = product_in.at[u, x, pl.ds(start, min(GROUP, rings - start))]
            remote(arrived, arrived, back_send.at[u], back_recv.at[u, g], twin).wait_recv()
            begin = start if g else 0
            part = product_in.at[u, x, pl.ds(begin, min(start + GROUP, rings) - begin)]
            for t in (2, 1, 3) if lanes_x == 4 else range(1, lanes_x):
                remote(part, part, lane_sem.at[u, 0], lane_sem.at[u, 1], {"chan": to_x(t)}).start()
        phase("lwait")
        many = product_in.at[u, pl.ds(0, lanes_x - 1)]
        lanes_all = remote(many, many, lane_sem.at[u, 0], lane_sem.at[u, 1], twin)
        lanes_all.wait_recv()
        closing.append(lanes_all.wait_send)

        phase("hidden")
        hidden = [
            nn(perm_back[...], product_in[u, lane].reshape(size, LANES)) for lane in range(lanes_x)
        ]
        for m in range(blocks):
            block = jnp.concatenate([part[m * rings : (m + 1) * rings] for part in hidden], axis=0)
            block = (norm_rows(block) * columns[u, 2]).astype(BF16)
            update = nn(out_weights[u], block)
            value = pair[m] + gating[m] * update
            if u == 0:
                pair[m] = value.astype(BF16).astype(F32)
            else:
                r, jh = m // per_row, m % per_row
                out_ref[r, jh * LANES : (jh + 1) * LANES, :] = jnp.transpose(value).astype(BF16)

    phase("close")
    for wait in closing:
        wait()
    phase(None)


def body(
    prior_pair,
    single,
    target,
    residue_mask,
    recycle_gain,
    recycle_bias,
    left_single,
    right_single,
    left_target,
    right_target,
    tri_gain,
    tri_proj,
    tri_gate,
    tri_gate_bias,
    tri_out_gain,
    tri_out,
):
    rings = lax.axis_size("dap") // 2
    lanes_x = lax.axis_size("chan")
    rows, cols, depth = prior_pair.shape
    blocks = rows * cols // LANES
    size = rings * blocks
    groups = -(-(rings - 1) // GROUP)
    vmem = pl.BlockSpec(memory_space=pltpu.VMEM)
    hbm = pl.BlockSpec(memory_space=pltpu.HBM)
    dma = pltpu.SemaphoreType.DMA
    operands = (
        prior_pair,
        single,
        target,
        residue_mask,
        recycle_gain[None, :],
        recycle_bias[None, :],
        left_single,
        right_single,
        left_target,
        right_target,
        tri_gain,
        tri_proj,
        tri_gate,
        tri_gate_bias,
        tri_out_gain,
        tri_out,
    )
    held = [
        pltpu.SMEM(a.shape, a.dtype) if a.dtype == jnp.int32 else pltpu.VMEM(a.shape, a.dtype)
        for a in operands
    ]
    return pl.pallas_call(
        functools.partial(kernel, rings, lanes_x),
        out_shape=jax.ShapeDtypeStruct(prior_pair.shape, BF16),
        in_specs=[hbm] * len(operands),
        out_specs=vmem,
        scratch_shapes=held
        + [
            pltpu.VMEM((2, rings, 2 * rows, LANES), F32),
            pltpu.VMEM((2, rings, 2, blocks, LANES), BF16),
            pltpu.VMEM((2, 2, rings, 2, blocks, LANES), BF16),
            pltpu.VMEM((2, rings, blocks, LANES), BF16),
            pltpu.VMEM((2, lanes_x, rings, blocks, LANES), BF16),
            pltpu.VMEM((blocks, depth, LANES), F32),
            pltpu.VMEM((blocks, depth, LANES), F32),
            pltpu.VMEM((blocks, depth, LANES), BF16),
            pltpu.VMEM((2, 4, depth, depth), BF16),
            pltpu.VMEM((2, depth, depth), BF16),
            pltpu.VMEM((2, depth, depth), BF16),
            pltpu.VMEM((2, 3, depth, LANES), F32),
            pltpu.VMEM((size, size), BF16),
            pltpu.VMEM((size, size), BF16),
            pltpu.VMEM((2, size, size), BF16),
            pltpu.VMEM((2, size, 2 * size), BF16),
            pltpu.VMEM((size, cols), BF16),
            dma((len(operands),)),
            dma((1,)),
            dma((rings,)),
            dma((2, 2)),
            dma((2,)),
            dma((2, groups)),
            dma((3,)),
            dma((3,)),
            dma((2, 2)),
        ],
        compiler_params=pltpu.CompilerParams(collective_id=0, has_side_effects=True),
        name="triangles",
    )(*operands)


def solution(mesh):
    rows = P(("crops", "dap"))
    placed = (P(("crops", "dap"), None, None), P(("crops", "dap"), None), rows, rows) + (P(),) * 12
    return jax.shard_map(
        body, mesh=mesh, in_specs=placed, out_specs=P(("crops", "dap"), None, None), check_vma=False
    )
```

```python
import functools

import jax
import jax.numpy as jnp
from jax import lax
from jax.experimental import pallas as pl
from jax.experimental.pallas import tpu as pltpu
from jax.sharding import PartitionSpec as P

F32 = jnp.float32
BF16 = jnp.bfloat16
MESH = pl.DeviceIdType.MESH
EPS = 1e-05
LANES = 128
GROUP = 8
STRIDE = 4
TAIL = 29
EARLY = 1


def selection(shape, column_of_row):
    rows = lax.broadcasted_iota(jnp.int32, shape, 0)
    columns = lax.broadcasted_iota(jnp.int32, shape, 1)
    return jnp.where(columns == column_of_row(rows), 1.0, 0.0).astype(BF16)


def nn(a, b):
    return lax.dot_general(a, b, (((1,), (0,)), ((), ())), preferred_element_type=F32)


def nt(a, b):
    return lax.dot_general(a, b, (((1,), (1,)), ((), ())), preferred_element_type=F32)


def norm_rows(values):
    scale = 1.0 / values.shape[0]
    center = values - jnp.sum(values, axis=0, keepdims=True) * scale
    spread = jnp.sum(center * center, axis=0, keepdims=True) * scale
    return center * lax.rsqrt(spread + EPS)


class Phases:
    def __init__(self):
        self.scope = None

    def __call__(self, name):
        if self.scope is not None:
            self.scope.__exit__(None, None, None)
        self.scope = jax.named_scope(name) if name else None
        if self.scope is not None:
            self.scope.__enter__()


def column(row_vector):
    return jnp.transpose(jnp.broadcast_to(row_vector, (LANES, LANES)))


def kernel(
    rings,
    lanes_x,
    prior_hbm,
    single_hbm,
    target_hbm,
    mask_hbm,
    recycle_gain_hbm,
    recycle_bias_hbm,
    left_single_hbm,
    right_single_hbm,
    left_target_hbm,
    right_target_hbm,
    tri_gain_hbm,
    tri_proj_hbm,
    tri_gate_hbm,
    tri_gate_bias_hbm,
    tri_out_gain_hbm,
    tri_out_hbm,
    out_ref,
    prior_ref,
    single_ref,
    target_ref,
    mask_ref,
    recycle_gain_ref,
    recycle_bias_ref,
    left_single_ref,
    right_single_ref,
    left_target_ref,
    right_target_ref,
    tri_gain_ref,
    tri_proj_ref,
    tri_gate_ref,
    tri_gate_bias_ref,
    tri_out_gain_ref,
    tri_out_ref,
    terms,
    edges_out,
    edges_in,
    product_out,
    product_in,
    base,
    pair,
    normed,
    weights,
    gate_weights,
    out_weights,
    columns,
    perm,
    perm_back,
    pick,
    pick_right,
    pick_left,
    load_sem,
    terms_send,
    terms_recv,
    edge_sem,
    back_send,
    back_recv,
    twin_send,
    twin_recv,
    lane_sem,
):
    rows, cols, depth = prior_ref.shape
    blocks = rows * cols // LANES
    per_row = cols // LANES
    width = depth // lanes_x
    size = rings * blocks
    dap = lax.axis_index("dap")
    x = lax.axis_index("chan")
    z = dap // 2
    h = lax.rem(dap, 2)
    twin = {"dap": dap + 1 - 2 * h}
    phase = Phases()

    def offset(p):
        up = (p + 1) // 2
        return rings + up * (2 * lax.rem(p, 2) - 1)

    def to_z(peer):
        return {"dap": 2 * peer + h}

    def to_x(t):
        return lax.rem(x + t, lanes_x)

    phase("greet")
    barrier = pltpu.get_barrier_semaphore()

    q = lax.rem(z + rings - 1, rings)
    last = rings - 1

    def at(order):
        return to_z(lax.rem(order + 1, rings))

    def greet(order):
        pl.semaphore_signal(barrier, inc=1, device_id=at(order), device_id_type=MESH)

    for back in range(1, STRIDE + 1):
        pl.when(q >= back)(functools.partial(greet, q - back))
    pl.semaphore_signal(barrier, inc=1, device_id=twin, device_id_type=MESH)
    for t in range(1, lanes_x):
        pl.semaphore_signal(barrier, inc=1, device_id={"chan": to_x(t)}, device_id_type=MESH)

    sources = (
        (single_hbm, single_ref),
        (right_single_hbm, right_single_ref),
        (target_hbm, target_ref),
        (mask_hbm, mask_ref),
        (right_target_hbm, right_target_ref),
        (left_single_hbm, left_single_ref),
        (left_target_hbm, left_target_ref),
        (recycle_gain_hbm, recycle_gain_ref),
        (recycle_bias_hbm, recycle_bias_ref),
        (prior_hbm, prior_ref),
        (tri_proj_hbm, tri_proj_ref),
        (tri_gain_hbm, tri_gain_ref),
        (tri_gate_hbm, tri_gate_ref),
        (tri_gate_bias_hbm, tri_gate_bias_ref),
        (tri_out_gain_hbm, tri_out_gain_ref),
        (tri_out_hbm, tri_out_ref),
    )
    loads = [
        pltpu.make_async_copy(source, held, load_sem.at[n])
        for n, (source, held) in enumerate(sources)
    ]
    for load in loads:
        load.start()

    def greet_later(order, carry):
        greet(order)
        return carry

    lax.fori_loop(q + 1, rings, greet_later, 0)

    phase("terms")
    for load in loads[:5]:
        load.wait()
    single = single_ref[...]
    mask_of = [mask_ref[r].astype(F32) for r in range(rows)]

    def row_terms(weight_ref, table_ref):
        linear = nn(single, weight_ref[...])
        table = table_ref[...].astype(F32)
        classes = lax.broadcasted_iota(jnp.int32, table.shape, 0)
        picked = [
            jnp.sum(jnp.where(classes == target_ref[r], table, 0.0), axis=0, keepdims=True)
            for r in range(rows)
        ]
        return [linear[r : r + 1] + picked[r] for r in range(rows)]

    right_rows = row_terms(right_single_ref, right_target_ref)
    mask_rows = [jnp.full((1, depth), mask_of[r], F32) for r in range(rows)]
    tile = jnp.concatenate(right_rows + mask_rows, axis=0)
    terms[h, z] = jnp.where(h == 0, tile, pltpu.roll(tile, rows, 0))

    phase("barrier")
    pl.semaphore_wait(barrier, q + jnp.minimum(STRIDE, last - q) + 1 + lanes_x - 1)

    def remote(source, target, send, recv, device):
        return pltpu.make_async_remote_copy(
            src_ref=source,
            dst_ref=target,
            send_sem=send,
            recv_sem=recv,
            device_id=device,
            device_id_type=MESH,
        )

    closing = []
    starts = [*range(1, TAIL, GROUP), TAIL]
    spans = list(zip(starts, starts[1:] + [rings]))

    def group_of(p):
        return (p - 1) // GROUP + jnp.where(p >= TAIL, 1, 0)

    phase("tsend")

    def give(source, order):
        tile = terms.at[h, source]
        remote(tile, tile, terms_send.at[0], terms_recv.at[source], at(order)).start()

    def carried(source):
        return lax.rem(source, lanes_x) == x

    for ahead in range(1, STRIDE + 1):
        pl.when(carried(z) & (q + ahead <= last))(functools.partial(give, z, q + ahead))

    def give_earlier(t, carry):
        order = lax.rem(q + offset(rings - 1 - t), rings)
        pl.when(order < q)(functools.partial(give, z, order))
        return carry

    lax.fori_loop(0, rings - 1, give_earlier, 0)

    def await_terms(source):
        tile = terms.at[h, source]
        remote(tile, tile, terms_send.at[0], terms_recv.at[source], twin).wait_recv()

    early = q + STRIDE <= last

    def lower(order):
        return lax.rem(order + 1, rings)

    def hand_over(source):
        tile = terms.at[h, source]
        for lane in range(1, lanes_x):
            to = {"chan": to_x(lane)}
            remote(tile, tile, terms_send.at[0], terms_recv.at[source], to).start()

    def relay(order, carry):
        source = lower(order)

        @pl.when(carried(source))
        def _():
            await_terms(source)
            pl.when(early)(functools.partial(give, source, q + STRIDE))
            pl.when(jnp.logical_not(early))(functools.partial(hand_over, source))

        return carry

    def hand_over_all(order, carry):
        source = lower(order)
        pl.when(carried(source))(functools.partial(hand_over, source))
        return carry

    def relay_all():
        lax.fori_loop(0, q, relay, 0)
        lax.fori_loop(0, jnp.where(early, q, 0), hand_over_all, 0)

    def collect(order, carry):
        source = lower(order)
        pl.when(jnp.logical_not(carried(source)))(functools.partial(await_terms, source))
        return carry

    def prepare():
        for load in loads[5:]:
            load.wait()
        left_rows = row_terms(left_single_ref, left_target_ref)
        gain = recycle_gain_ref[...]
        bias = recycle_bias_ref[...]
        for r in range(rows):
            for jh in range(per_row):
                block = prior_ref[r, jh * LANES : (jh + 1) * LANES, :].astype(F32)
                center = block - jnp.mean(block, axis=1, keepdims=True)
                spread = jnp.mean(center * center, axis=1, keepdims=True)
                value = center * lax.rsqrt(spread + EPS) * gain + bias + left_rows[r]
                base[r * per_row + jh] = jnp.transpose(value)
        for u in range(2):
            whole = tri_proj_ref[u].astype(F32)
            for g in range(4):
                weights[u, g] = jnp.transpose(whole[:, g, :]).astype(BF16)
            gate_weights[u] = jnp.transpose(tri_gate_ref[u].astype(F32)).astype(BF16)
            out_weights[u] = jnp.transpose(tri_out_ref[u].astype(F32)).astype(BF16)
            columns[u, 0] = column(tri_gain_ref[u : u + 1, :])
            columns[u, 1] = column(tri_gate_bias_ref[u : u + 1, :])
            columns[u, 2] = column(tri_out_gain_ref[u : u + 1, :])

        def place(channel):
            delta = lax.rem(channel - z + rings, rings)
            after = jnp.where(delta <= rings // 2, 2 * delta - 1, 2 * (rings - delta))
            return jnp.where(delta == 0, 0, after)

        perm[...] = selection((size, size), lambda q: lax.rem(q, blocks) * rings + q // blocks)
        perm_back[...] = selection(
            (size, size), lambda q: place(lax.rem(q, rings)) * blocks + q // rings
        )
        for half in range(2):
            pick[half] = selection((size, size), lambda q: q - lax.rem(q, 2) + half)
            pick_right[half] = selection(
                (size, 2 * size),
                lambda j: lax.rem(j // rows, 2) * size
                + (j // (2 * rows)) * blocks
                + 2 * lax.rem(j, rows)
                + half,
            )
        pick_left[...] = selection(
            (size, cols), lambda q: (q // blocks) * 2 * rows + rows * h + lax.rem(q, blocks) // 2
        )

    phase("relay")

    def turn(step, carry):
        pl.when((step == 0) == early)(relay_all)
        pl.when((step == 1) == early)(prepare)
        return carry

    lax.fori_loop(0, 2, turn, 0)

    phase("twait")
    def later(order, carry):
        await_terms(lax.rem(order + 1, rings))
        return carry

    lax.fori_loop(0, q, collect, 0)
    lax.fori_loop(q + 1, rings, later, 0)
    phase("ttwin")

    def swap(view, k):
        def copy(parity):
            return remote(view(parity), view(parity), twin_send.at[k], twin_recv.at[k], twin)

        copy(h).start()
        closing.append(copy(h).wait_send)
        copy(1 - h).wait_recv()

    swap(lambda parity: terms.at[parity], 0)

    phase("pair")
    first, second = terms[0], terms[1]
    upper = lax.broadcasted_iota(jnp.int32, first.shape, 1) < rows
    right_whole = jnp.where(upper, first, second).reshape(cols, depth)
    mask_whole = jnp.where(upper, second, first)
    mask_whole = pltpu.roll(mask_whole, rows, 1).reshape(cols, depth)
    masks = []
    for jh in range(per_row):
        right_t = jnp.transpose(right_whole[jh * LANES : (jh + 1) * LANES])
        masks.append(jnp.transpose(mask_whole[jh * LANES : (jh + 1) * LANES])[:1])
        for r in range(rows):
            m = r * per_row + jh
            pair[m] = (base[m] + right_t).astype(BF16).astype(F32)

    for u in range(2):
        phase("edges")
        local = [
            weights[u, g, pl.ds(pl.multiple_of(x * width, width), width), :] for g in range(4)
        ]
        local = jnp.concatenate(local, axis=0)
        left_parts, right_parts = [], []
        for m in range(blocks):
            block = (norm_rows(pair[m]) * columns[u, 0]).astype(BF16)
            normed[m] = block
            projected = nn(local, block)
            masked = masks[m % per_row] * mask_of[m // per_row]
            value, gate = projected[:width], projected[width : 2 * width]
            left_parts.append((masked * jax.nn.sigmoid(gate) * value).astype(BF16))
            value, gate = projected[2 * width : 3 * width], projected[3 * width :]
            right_parts.append((masked * jax.nn.sigmoid(gate) * value).astype(BF16))
        for side, parts in enumerate((left_parts, right_parts)):
            ordered = nn(perm[...], jnp.concatenate(parts, axis=0)).astype(BF16)
            edges_out[u, :, side] = ordered.reshape(rings, blocks, LANES)

        phase("esend")

        def send_edges(t, carry, u=u):
            peer = lax.rem(z + offset(rings - 1 - t), rings)
            remote(
                edges_out.at[u, peer],
                edges_in.at[u, h, z],
                edge_sem.at[u, 0],
                edge_sem.at[u, 1],
                to_z(peer),
            ).start()
            return carry

        lax.fori_loop(0, rings - 1, send_edges, 0)
        edges_in[u, h, z] = edges_out[u, z]
        gating = [
            jax.nn.sigmoid(nn(gate_weights[u], normed[m]) + columns[u, 1]) for m in range(blocks)
        ]
        many = edges_in.at[u, h, pl.ds(0, rings - 1)]
        edges_all = remote(many, many, edge_sem.at[u, 0], edge_sem.at[u, 1], twin)
        closing.append(edges_all.wait_send)
        if u == 0:
            relayed = (q - x + lanes_x) // lanes_x - jnp.where(x == 0, 1, 0)
            copies = lanes_x - 1 + jnp.where(q + STRIDE <= last, 1, 0)
            ahead = jnp.where(carried(z), jnp.minimum(STRIDE, last - q), 0)
            given = ahead + q + relayed * copies

            def gone(t, carry):
                tile = terms.at[h, z]
                remote(tile, tile, terms_send.at[0], terms_recv.at[z], twin).wait_send()
                return carry

            lax.fori_loop(0, given, gone, 0)
        phase("ewait")
        edges_all.wait_recv()
        phase("etwin")
        if u == 0:
            swap(lambda parity: edges_in.at[0, parity, :, 1], 1)
        else:
            swap(lambda parity: edges_in.at[1, parity], 2)

        phase("product")
        right_rows_all = edges_in[u, :, :, 1].reshape(2 * size, LANES)
        if u == 0:
            left_own = edges_in[u, h, :, 0].reshape(size, LANES)
            a = [nn(pick[half], left_own).astype(BF16) for half in range(2)]
            b = [nn(pick_right[half], right_rows_all).astype(BF16) for half in range(2)]
            whole = nt(jnp.concatenate(a, axis=1), jnp.concatenate(b, axis=1))
            even = lax.rem(lax.broadcasted_iota(jnp.int32, (size, LANES), 0), 2) == 0
            product = jnp.where(even, whole[:, :LANES], whole[:, LANES:])
        else:
            spread = []
            for parity in range(2):
                block = edges_in[u, parity, :, 0].reshape(size, LANES)
                halves = [nn(pick[half], block).astype(BF16) for half in range(2)]
                spread.append(jnp.concatenate(halves, axis=1))
            chosen = nt(pick_left[...], jnp.concatenate(spread, axis=0))
            row_half = lax.rem(lax.broadcasted_iota(jnp.int32, chosen.shape, 0), 2)
            column_half = lax.rem(lax.broadcasted_iota(jnp.int32, chosen.shape, 1), 2)
            chosen = jnp.where(row_half == column_half, chosen, 0.0).astype(BF16)
            product = nn(chosen, right_rows_all)
        product_out[u] = product.astype(BF16).reshape(rings, blocks, LANES)

        phase("bsend")

        def send_back(t, carry, u=u):
            p = rings - 1 - t
            peer = lax.rem(z + 2 * rings - offset(p), rings)

            def send(lane):
                remote(
                    product_out.at[u, peer],
                    product_in.at[u, x, p],
                    back_send.at[u],
                    lane_sem.at[u, 1] if lane else back_recv.at[u, group_of(p)],
                    {"dap": 2 * peer + h, "chan": to_x(lane)} if lane else to_z(peer),
                ).start()

            send(0)
            if u:

                @pl.when(peer < EARLY)
                def _():
                    for lane in range(1, lanes_x):
                        send(lane)

            return carry

        lax.fori_loop(0, rings - 1, send_back, 0)
        product_in[u, x, 0] = product_out[u, z]
        phase("bwait")
        direct = z < EARLY

        def forward(part, u=u):
            for t in (2, 1, 3) if lanes_x == 4 else range(1, lanes_x):
                remote(part, part, lane_sem.at[u, 0], lane_sem.at[u, 1], {"chan": to_x(t)}).start()

        def sent_back(many, times, u=u):
            def gone(t, carry):
                remote(many, many, back_send.at[u], back_recv.at[u, 0], twin).wait_send()
                return carry

            return functools.partial(lax.fori_loop, 0, times, gone, 0)

        closing.append(sent_back(product_out.at[u, pl.ds(0, rings - 1)], 1))
        if u:
            elsewhere = EARLY - jnp.where(direct, 1, 0)
            closing.append(sent_back(product_out.at[u, 0], elsewhere * (lanes_x - 1)))
            pl.when(direct)(functools.partial(forward, product_in.at[u, x, 0]))
        for g, (start, stop) in enumerate(spans):
            arrived = product_in.at[u, x, pl.ds(start, stop - start)]
            remote(arrived, arrived, back_send.at[u], back_recv.at[u, g], twin).wait_recv()
            begin = start if g else 0
            part = product_in.at[u, x, pl.ds(begin, stop - begin)]
            if u:
                pl.when(jnp.logical_not(direct))(functools.partial(forward, part))
            else:
                forward(part)
        phase("lwait")
        many = product_in.at[u, pl.ds(0, lanes_x - 1)]
        remote(many, many, lane_sem.at[u, 0], lane_sem.at[u, 1], twin).wait_recv()

        def sent_on(count, u=u):
            many = product_in.at[u, pl.ds(0, lanes_x - 1), pl.ds(0, count)]
            remote(many, many, lane_sem.at[u, 0], lane_sem.at[u, 1], twin).wait_send()

        one_sent, all_sent = functools.partial(sent_on, 1), functools.partial(sent_on, rings)
        if u:
            closing.append(functools.partial(pl.when(direct), one_sent))
            closing.append(functools.partial(pl.when(jnp.logical_not(direct)), all_sent))
        else:
            closing.append(all_sent)

        phase("hidden")
        hidden = [
            nn(perm_back[...], product_in[u, lane].reshape(size, LANES)) for lane in range(lanes_x)
        ]
        for m in range(blocks):
            block = jnp.concatenate([part[m * rings : (m + 1) * rings] for part in hidden], axis=0)
            block = (norm_rows(block) * columns[u, 2]).astype(BF16)
            update = nn(out_weights[u], block)
            value = pair[m] + gating[m] * update
            if u == 0:
                pair[m] = value.astype(BF16).astype(F32)
            else:
                r, jh = m // per_row, m % per_row
                out_ref[r, jh * LANES : (jh + 1) * LANES, :] = jnp.transpose(value).astype(BF16)

    phase("close")
    for wait in closing:
        wait()
    phase(None)


def body(
    prior_pair,
    single,
    target,
    residue_mask,
    recycle_gain,
    recycle_bias,
    left_single,
    right_single,
    left_target,
    right_target,
    tri_gain,
    tri_proj,
    tri_gate,
    tri_gate_bias,
    tri_out_gain,
    tri_out,
):
    rings = lax.axis_size("dap") // 2
    lanes_x = lax.axis_size("chan")
    rows, cols, depth = prior_pair.shape
    blocks = rows * cols // LANES
    size = rings * blocks
    groups = -(-(TAIL - 1) // GROUP) + 1
    vmem = pl.BlockSpec(memory_space=pltpu.VMEM)
    hbm = pl.BlockSpec(memory_space=pltpu.HBM)
    dma = pltpu.SemaphoreType.DMA
    operands = (
        prior_pair,
        single,
        target,
        residue_mask,
        recycle_gain[None, :],
        recycle_bias[None, :],
        left_single,
        right_single,
        left_target,
        right_target,
        tri_gain,
        tri_proj,
        tri_gate,
        tri_gate_bias,
        tri_out_gain,
        tri_out,
    )
    held = [
        pltpu.SMEM(a.shape, a.dtype) if a.dtype == jnp.int32 else pltpu.VMEM(a.shape, a.dtype)
        for a in operands
    ]
    return pl.pallas_call(
        functools.partial(kernel, rings, lanes_x),
        out_shape=pltpu.VMEM(prior_pair.shape, BF16),
        in_specs=[hbm] * len(operands),
        out_specs=vmem,
        scratch_shapes=held
        + [
            pltpu.VMEM((2, rings, 2 * rows, LANES), F32),
            pltpu.VMEM((2, rings, 2, blocks, LANES), BF16),
            pltpu.VMEM((2, 2, rings, 2, blocks, LANES), BF16),
            pltpu.VMEM((2, rings, blocks, LANES), BF16),
            pltpu.VMEM((2, lanes_x, rings, blocks, LANES), BF16),
            pltpu.VMEM((blocks, depth, LANES), F32),
            pltpu.VMEM((blocks, depth, LANES), F32),
            pltpu.VMEM((blocks, depth, LANES), BF16),
            pltpu.VMEM((2, 4, depth, depth), BF16),
            pltpu.VMEM((2, depth, depth), BF16),
            pltpu.VMEM((2, depth, depth), BF16),
            pltpu.VMEM((2, 3, depth, LANES), F32),
            pltpu.VMEM((size, size), BF16),
            pltpu.VMEM((size, size), BF16),
            pltpu.VMEM((2, size, size), BF16),
            pltpu.VMEM((2, size, 2 * size), BF16),
            pltpu.VMEM((size, cols), BF16),
            dma((len(operands),)),
            dma((1,)),
            dma((rings,)),
            dma((2, 2)),
            dma((2,)),
            dma((2, groups)),
            dma((3,)),
            dma((3,)),
            dma((2, 2)),
        ],
        compiler_params=pltpu.CompilerParams(collective_id=0, has_side_effects=True),
        name="triangles",
    )(*operands)


def solution(mesh):
    rows = P(("crops", "dap"))
    placed = (P(("crops", "dap"), None, None), P(("crops", "dap"), None), rows, rows) + (P(),) * 12
    return jax.shard_map(
        body, mesh=mesh, in_specs=placed, out_specs=P(("crops", "dap"), None, None), check_vma=False
    )
```

```python
import functools

import jax
import jax.numpy as jnp
from jax import lax
from jax.experimental import pallas as pl
from jax.experimental.pallas import tpu as pltpu
from jax.sharding import PartitionSpec as P

F32 = jnp.float32
BF16 = jnp.bfloat16
MESH = pl.DeviceIdType.MESH
EPS = 1e-05
LANES = 128
GROUP = 8
STRIDE = 4
TAIL = 29
EARLY = 1


def selection(shape, column_of_row):
    rows = lax.broadcasted_iota(jnp.int32, shape, 0)
    columns = lax.broadcasted_iota(jnp.int32, shape, 1)
    return jnp.where(columns == column_of_row(rows), 1.0, 0.0).astype(BF16)


def nn(a, b):
    return lax.dot_general(a, b, (((1,), (0,)), ((), ())), preferred_element_type=F32)


def nt(a, b):
    return lax.dot_general(a, b, (((1,), (1,)), ((), ())), preferred_element_type=F32)


def norm_rows(values):
    scale = 1.0 / values.shape[0]
    center = values - jnp.sum(values, axis=0, keepdims=True) * scale
    spread = jnp.sum(center * center, axis=0, keepdims=True) * scale
    return center * lax.rsqrt(spread + EPS)


class Phases:
    def __init__(self):
        self.scope = None

    def __call__(self, name):
        if self.scope is not None:
            self.scope.__exit__(None, None, None)
        self.scope = jax.named_scope(name) if name else None
        if self.scope is not None:
            self.scope.__enter__()


def column(row_vector):
    return jnp.transpose(jnp.broadcast_to(row_vector, (LANES, LANES)))


def kernel(
    rings,
    lanes_x,
    prior_hbm,
    single_hbm,
    target_hbm,
    mask_hbm,
    recycle_gain_hbm,
    recycle_bias_hbm,
    left_single_hbm,
    right_single_hbm,
    left_target_hbm,
    right_target_hbm,
    tri_gain_hbm,
    tri_proj_hbm,
    tri_gate_hbm,
    tri_gate_bias_hbm,
    tri_out_gain_hbm,
    tri_out_hbm,
    out_ref,
    prior_ref,
    single_ref,
    target_ref,
    mask_ref,
    recycle_gain_ref,
    recycle_bias_ref,
    left_single_ref,
    right_single_ref,
    left_target_ref,
    right_target_ref,
    tri_gain_ref,
    tri_proj_ref,
    tri_gate_ref,
    tri_gate_bias_ref,
    tri_out_gain_ref,
    tri_out_ref,
    terms,
    right_all,
    edges_out,
    edges_in,
    product_out,
    product_in,
    base,
    pair,
    normed,
    weights,
    gate_weights,
    out_weights,
    columns,
    perm,
    perm_back,
    pick,
    pick_right,
    pick_left,
    load_sem,
    terms_send,
    terms_recv,
    edge_sem,
    back_send,
    back_recv,
    twin_send,
    twin_recv,
    lane_sem,
):
    rows, cols, depth = prior_ref.shape
    blocks = rows * cols // LANES
    per_row = cols // LANES
    width = depth // lanes_x
    size = rings * blocks
    dap = lax.axis_index("dap")
    x = lax.axis_index("chan")
    z = dap // 2
    h = lax.rem(dap, 2)
    twin = {"dap": dap + 1 - 2 * h}
    phase = Phases()

    def offset(p):
        up = (p + 1) // 2
        return rings + up * (2 * lax.rem(p, 2) - 1)

    def to_z(peer):
        return {"dap": 2 * peer + h}

    def to_x(t):
        return lax.rem(x + t, lanes_x)

    phase("greet")
    barrier = pltpu.get_barrier_semaphore()

    q = lax.rem(z + rings - 1, rings)
    last = rings - 1

    def at(order):
        return to_z(lax.rem(order + 1, rings))

    def greet(order):
        pl.semaphore_signal(barrier, inc=1, device_id=at(order), device_id_type=MESH)

    for back in range(1, STRIDE + 1):
        pl.when(q >= back)(functools.partial(greet, q - back))
    pl.semaphore_signal(barrier, inc=1, device_id=twin, device_id_type=MESH)
    for t in range(1, lanes_x):
        pl.semaphore_signal(barrier, inc=1, device_id={"chan": to_x(t)}, device_id_type=MESH)

    sources = (
        (single_hbm, single_ref),
        (right_single_hbm, right_single_ref),
        (target_hbm, target_ref),
        (mask_hbm, mask_ref),
        (right_target_hbm, right_target_ref),
        (left_single_hbm, left_single_ref),
        (left_target_hbm, left_target_ref),
        (recycle_gain_hbm, recycle_gain_ref),
        (recycle_bias_hbm, recycle_bias_ref),
        (prior_hbm, prior_ref),
        (tri_proj_hbm, tri_proj_ref),
        (tri_gain_hbm, tri_gain_ref),
        (tri_gate_hbm, tri_gate_ref),
        (tri_gate_bias_hbm, tri_gate_bias_ref),
        (tri_out_gain_hbm, tri_out_gain_ref),
        (tri_out_hbm, tri_out_ref),
    )
    loads = [
        pltpu.make_async_copy(source, held, load_sem.at[n])
        for n, (source, held) in enumerate(sources)
    ]
    for load in loads:
        load.start()

    def greet_later(order, carry):
        greet(order)
        return carry

    lax.fori_loop(q + 1, rings, greet_later, 0)

    phase("terms")
    for load in loads[:5]:
        load.wait()
    single = single_ref[...]
    mask_of = [mask_ref[r].astype(F32) for r in range(rows)]

    def row_terms(weight_ref, table_ref):
        linear = nn(single, weight_ref[...])
        table = table_ref[...].astype(F32)
        classes = lax.broadcasted_iota(jnp.int32, table.shape, 0)
        picked = [
            jnp.sum(jnp.where(classes == target_ref[r], table, 0.0), axis=0, keepdims=True)
            for r in range(rows)
        ]
        return [linear[r : r + 1] + picked[r] for r in range(rows)]

    right_rows = row_terms(right_single_ref, right_target_ref)
    lane_row = lax.rem(lax.broadcasted_iota(jnp.int32, (1, LANES), 1), rows)
    mask_row = jnp.zeros((1, LANES), F32)
    for r in range(rows):
        mask_row = jnp.where(lane_row == r, mask_of[r], mask_row)
    for r, row in enumerate(right_rows + [mask_row]):
        terms[h, z, :, r * LANES : (r + 1) * LANES] = row

    phase("barrier")
    pl.semaphore_wait(barrier, q + jnp.minimum(STRIDE, last - q) + 1 + lanes_x - 1)

    def remote(source, target, send, recv, device):
        return pltpu.make_async_remote_copy(
            src_ref=source,
            dst_ref=target,
            send_sem=send,
            recv_sem=recv,
            device_id=device,
            device_id_type=MESH,
        )

    closing = []
    starts = [*range(1, TAIL, GROUP), TAIL]
    spans = list(zip(starts, starts[1:] + [rings]))

    def group_of(p):
        return (p - 1) // GROUP + jnp.where(p >= TAIL, 1, 0)

    phase("tsend")

    def give(source, order):
        tile = terms.at[h, source]
        remote(tile, tile, terms_send.at[0], terms_recv.at[source], at(order)).start()

    def carried(source):
        return lax.rem(source, lanes_x) == x

    for ahead in range(1, STRIDE + 1):
        pl.when(carried(z) & (q + ahead <= last))(functools.partial(give, z, q + ahead))

    def give_earlier(t, carry):
        order = lax.rem(q + offset(rings - 1 - t), rings)
        pl.when(order < q)(functools.partial(give, z, order))
        return carry

    lax.fori_loop(0, rings - 1, give_earlier, 0)

    def await_terms(source):
        tile = terms.at[h, source]
        remote(tile, tile, terms_send.at[0], terms_recv.at[source], twin).wait_recv()

    early = q + STRIDE <= last

    def lower(order):
        return lax.rem(order + 1, rings)

    def hand_over(source):
        tile = terms.at[h, source]
        for lane in range(1, lanes_x):
            to = {"chan": to_x(lane)}
            remote(tile, tile, terms_send.at[0], terms_recv.at[source], to).start()

    def relay(order, carry):
        source = lower(order)

        @pl.when(carried(source))
        def _():
            await_terms(source)
            pl.when(early)(functools.partial(give, source, q + STRIDE))
            pl.when(jnp.logical_not(early))(functools.partial(hand_over, source))

        return carry

    def hand_over_all(order, carry):
        source = lower(order)
        pl.when(carried(source))(functools.partial(hand_over, source))
        return carry

    def relay_all():
        lax.fori_loop(0, q, relay, 0)
        lax.fori_loop(0, jnp.where(early, q, 0), hand_over_all, 0)

    def collect(order, carry):
        source = lower(order)
        pl.when(jnp.logical_not(carried(source)))(functools.partial(await_terms, source))
        return carry

    def prepare():
        for load in loads[5:]:
            load.wait()
        left_rows = row_terms(left_single_ref, left_target_ref)
        gain = recycle_gain_ref[...]
        bias = recycle_bias_ref[...]
        for r in range(rows):
            for jh in range(per_row):
                block = prior_ref[r, jh * LANES : (jh + 1) * LANES, :].astype(F32)
                center = block - jnp.mean(block, axis=1, keepdims=True)
                spread = jnp.mean(center * center, axis=1, keepdims=True)
                value = center * lax.rsqrt(spread + EPS) * gain + bias + left_rows[r]
                base[r * per_row + jh] = jnp.transpose(value)
        for u in range(2):
            whole = tri_proj_ref[u].astype(F32)
            for g in range(4):
                weights[u, g] = jnp.transpose(whole[:, g, :]).astype(BF16)
            gate_weights[u] = jnp.transpose(tri_gate_ref[u].astype(F32)).astype(BF16)
            out_weights[u] = jnp.transpose(tri_out_ref[u].astype(F32)).astype(BF16)
            columns[u, 0] = column(tri_gain_ref[u : u + 1, :])
            columns[u, 1] = column(tri_gate_bias_ref[u : u + 1, :])
            columns[u, 2] = column(tri_out_gain_ref[u : u + 1, :])

        def place(channel):
            delta = lax.rem(channel - z + rings, rings)
            after = jnp.where(delta <= rings // 2, 2 * delta - 1, 2 * (rings - delta))
            return jnp.where(delta == 0, 0, after)

        perm[...] = selection((size, size), lambda q: lax.rem(q, blocks) * rings + q // blocks)
        perm_back[...] = selection(
            (size, size), lambda q: place(lax.rem(q, rings)) * blocks + q // rings
        )
        for half in range(2):
            pick[half] = selection((size, size), lambda q: q - lax.rem(q, 2) + half)
            pick_right[half] = selection(
                (size, 2 * size),
                lambda j: lax.rem(j // rows, 2) * size
                + (j // (2 * rows)) * blocks
                + 2 * lax.rem(j, rows)
                + half,
            )
        pick_left[...] = selection(
            (size, cols), lambda q: (q // blocks) * 2 * rows + rows * h + lax.rem(q, blocks) // 2
        )

    phase("relay")

    def turn(step, carry):
        pl.when((step == 0) == early)(relay_all)
        pl.when((step == 1) == early)(prepare)
        return carry

    lax.fori_loop(0, 2, turn, 0)

    phase("twait")
    def later(order, carry):
        await_terms(lax.rem(order + 1, rings))
        return carry

    lax.fori_loop(0, q, collect, 0)
    lax.fori_loop(q + 1, rings, later, 0)
    phase("ttwin")

    def swap(view, k):
        def copy(parity):
            return remote(view(parity), view(parity), twin_send.at[k], twin_recv.at[k], twin)

        copy(h).start()
        closing.append(copy(h).wait_send)
        copy(1 - h).wait_recv()

    swap(lambda parity: terms.at[parity], 0)

    phase("pair")
    for parity in range(2):
        for r in range(rows):
            part = terms[parity, :, 0, r * LANES : (r + 1) * LANES]
            right_all[:, parity * rows + r, :] = part
    right_whole = right_all[...].reshape(cols, depth)
    lane = lax.broadcasted_iota(jnp.int32, (rings, LANES), 1)
    source = lax.broadcasted_iota(jnp.int32, (rings, LANES), 0)
    first, second = (terms[parity, :, 0, rows * LANES :] for parity in range(2))
    mask_table = jnp.where(lax.rem(lane // rows, 2) == 0, first, second)
    masks = []
    for jh in range(per_row):
        right_t = jnp.transpose(right_whole[jh * LANES : (jh + 1) * LANES])
        chosen = source == (jh * LANES + lane) // (2 * rows)
        masks.append(jnp.sum(jnp.where(chosen, mask_table, 0.0), axis=0, keepdims=True))
        for r in range(rows):
            m = r * per_row + jh
            pair[m] = (base[m] + right_t).astype(BF16).astype(F32)

    for u in range(2):
        phase("edges")
        local = [
            weights[u, g, pl.ds(pl.multiple_of(x * width, width), width), :] for g in range(4)
        ]
        local = jnp.concatenate(local, axis=0)
        left_parts, right_parts = [], []
        for m in range(blocks):
            block = (norm_rows(pair[m]) * columns[u, 0]).astype(BF16)
            normed[m] = block
            projected = nn(local, block)
            masked = masks[m % per_row] * mask_of[m // per_row]
            value, gate = projected[:width], projected[width : 2 * width]
            left_parts.append((masked * jax.nn.sigmoid(gate) * value).astype(BF16))
            value, gate = projected[2 * width : 3 * width], projected[3 * width :]
            right_parts.append((masked * jax.nn.sigmoid(gate) * value).astype(BF16))
        for side, parts in enumerate((left_parts, right_parts)):
            ordered = nn(perm[...], jnp.concatenate(parts, axis=0)).astype(BF16)
            edges_out[u, :, side] = ordered.reshape(rings, blocks, LANES)

        phase("esend")

        def send_edges(t, carry, u=u):
            peer = lax.rem(z + offset(rings - 1 - t), rings)
            remote(
                edges_out.at[u, peer],
                edges_in.at[u, h, z],
                edge_sem.at[u, 0],
                edge_sem.at[u, 1],
                to_z(peer),
            ).start()
            return carry

        lax.fori_loop(0, rings - 1, send_edges, 0)
        edges_in[u, h, z] = edges_out[u, z]
        gating = [
            jax.nn.sigmoid(nn(gate_weights[u], normed[m]) + columns[u, 1]) for m in range(blocks)
        ]
        many = edges_in.at[u, h, pl.ds(0, rings - 1)]
        edges_all = remote(many, many, edge_sem.at[u, 0], edge_sem.at[u, 1], twin)
        closing.append(edges_all.wait_send)
        if u == 0:
            relayed = (q - x + lanes_x) // lanes_x - jnp.where(x == 0, 1, 0)
            copies = lanes_x - 1 + jnp.where(q + STRIDE <= last, 1, 0)
            ahead = jnp.where(carried(z), jnp.minimum(STRIDE, last - q), 0)
            given = ahead + q + relayed * copies

            def gone(t, carry):
                tile = terms.at[h, z]
                remote(tile, tile, terms_send.at[0], terms_recv.at[z], twin).wait_send()
                return carry

            lax.fori_loop(0, given, gone, 0)
        phase("ewait")
        edges_all.wait_recv()
        phase("etwin")
        if u == 0:
            swap(lambda parity: edges_in.at[0, parity, :, 1], 1)
        else:
            swap(lambda parity: edges_in.at[1, parity], 2)

        phase("product")
        right_rows_all = edges_in[u, :, :, 1].reshape(2 * size, LANES)
        if u == 0:
            left_own = edges_in[u, h, :, 0].reshape(size, LANES)
            a = [nn(pick[half], left_own).astype(BF16) for half in range(2)]
            b = [nn(pick_right[half], right_rows_all).astype(BF16) for half in range(2)]
            whole = nt(jnp.concatenate(a, axis=1), jnp.concatenate(b, axis=1))
            even = lax.rem(lax.broadcasted_iota(jnp.int32, (size, LANES), 0), 2) == 0
            product = jnp.where(even, whole[:, :LANES], whole[:, LANES:])
        else:
            spread = []
            for parity in range(2):
                block = edges_in[u, parity, :, 0].reshape(size, LANES)
                halves = [nn(pick[half], block).astype(BF16) for half in range(2)]
                spread.append(jnp.concatenate(halves, axis=1))
            chosen = nt(pick_left[...], jnp.concatenate(spread, axis=0))
            row_half = lax.rem(lax.broadcasted_iota(jnp.int32, chosen.shape, 0), 2)
            column_half = lax.rem(lax.broadcasted_iota(jnp.int32, chosen.shape, 1), 2)
            chosen = jnp.where(row_half == column_half, chosen, 0.0).astype(BF16)
            product = nn(chosen, right_rows_all)
        product_out[u] = product.astype(BF16).reshape(rings, blocks, LANES)

        phase("bsend")

        def send_back(t, carry, u=u):
            p = rings - 1 - t
            peer = lax.rem(z + 2 * rings - offset(p), rings)

            def send(lane):
                remote(
                    product_out.at[u, peer],
                    product_in.at[u, x, p],
                    back_send.at[u],
                    lane_sem.at[u, 1] if lane else back_recv.at[u, group_of(p)],
                    {"dap": 2 * peer + h, "chan": to_x(lane)} if lane else to_z(peer),
                ).start()

            send(0)
            if u:

                @pl.when(peer < EARLY)
                def _():
                    for lane in range(1, lanes_x):
                        send(lane)

            return carry

        lax.fori_loop(0, rings - 1, send_back, 0)
        product_in[u, x, 0] = product_out[u, z]
        phase("bwait")
        direct = z < EARLY

        def forward(part, u=u):
            for t in (2, 1, 3) if lanes_x == 4 else range(1, lanes_x):
                remote(part, part, lane_sem.at[u, 0], lane_sem.at[u, 1], {"chan": to_x(t)}).start()

        def sent_back(many, times, u=u):
            def gone(t, carry):
                remote(many, many, back_send.at[u], back_recv.at[u, 0], twin).wait_send()
                return carry

            return functools.partial(lax.fori_loop, 0, times, gone, 0)

        closing.append(sent_back(product_out.at[u, pl.ds(0, rings - 1)], 1))
        if u:
            elsewhere = EARLY - jnp.where(direct, 1, 0)
            closing.append(sent_back(product_out.at[u, 0], elsewhere * (lanes_x - 1)))
            pl.when(direct)(functools.partial(forward, product_in.at[u, x, 0]))
        for g, (start, stop) in enumerate(spans):
            arrived = product_in.at[u, x, pl.ds(start, stop - start)]
            remote(arrived, arrived, back_send.at[u], back_recv.at[u, g], twin).wait_recv()
            begin = start if g else 0
            part = product_in.at[u, x, pl.ds(begin, stop - begin)]
            if u:
                pl.when(jnp.logical_not(direct))(functools.partial(forward, part))
            else:
                forward(part)
        phase("lwait")
        many = product_in.at[u, pl.ds(0, lanes_x - 1)]
        remote(many, many, lane_sem.at[u, 0], lane_sem.at[u, 1], twin).wait_recv()

        def sent_on(count, u=u):
            many = product_in.at[u, pl.ds(0, lanes_x - 1), pl.ds(0, count)]
            remote(many, many, lane_sem.at[u, 0], lane_sem.at[u, 1], twin).wait_send()

        one_sent, all_sent = functools.partial(sent_on, 1), functools.partial(sent_on, rings)
        if u:
            closing.append(functools.partial(pl.when(direct), one_sent))
            closing.append(functools.partial(pl.when(jnp.logical_not(direct)), all_sent))
        else:
            closing.append(all_sent)

        phase("hidden")
        hidden = [
            nn(perm_back[...], product_in[u, lane].reshape(size, LANES)) for lane in range(lanes_x)
        ]
        for m in range(blocks):
            block = jnp.concatenate([part[m * rings : (m + 1) * rings] for part in hidden], axis=0)
            block = (norm_rows(block) * columns[u, 2]).astype(BF16)
            update = nn(out_weights[u], block)
            value = pair[m] + gating[m] * update
            if u == 0:
                pair[m] = value.astype(BF16).astype(F32)
            else:
                r, jh = m // per_row, m % per_row
                out_ref[r, jh * LANES : (jh + 1) * LANES, :] = jnp.transpose(value).astype(BF16)

    phase("close")
    for wait in closing:
        wait()
    phase(None)


def body(
    prior_pair,
    single,
    target,
    residue_mask,
    recycle_gain,
    recycle_bias,
    left_single,
    right_single,
    left_target,
    right_target,
    tri_gain,
    tri_proj,
    tri_gate,
    tri_gate_bias,
    tri_out_gain,
    tri_out,
):
    rings = lax.axis_size("dap") // 2
    lanes_x = lax.axis_size("chan")
    rows, cols, depth = prior_pair.shape
    blocks = rows * cols // LANES
    size = rings * blocks
    groups = -(-(TAIL - 1) // GROUP) + 1
    vmem = pl.BlockSpec(memory_space=pltpu.VMEM)
    hbm = pl.BlockSpec(memory_space=pltpu.HBM)
    dma = pltpu.SemaphoreType.DMA
    operands = (
        prior_pair,
        single,
        target,
        residue_mask,
        recycle_gain[None, :],
        recycle_bias[None, :],
        left_single,
        right_single,
        left_target,
        right_target,
        tri_gain,
        tri_proj,
        tri_gate,
        tri_gate_bias,
        tri_out_gain,
        tri_out,
    )
    held = [
        pltpu.SMEM(a.shape, a.dtype) if a.dtype == jnp.int32 else pltpu.VMEM(a.shape, a.dtype)
        for a in operands
    ]
    return pl.pallas_call(
        functools.partial(kernel, rings, lanes_x),
        out_shape=pltpu.VMEM(prior_pair.shape, BF16),
        in_specs=[hbm] * len(operands),
        out_specs=vmem,
        scratch_shapes=held
        + [
            pltpu.VMEM((2, rings, 1, (rows + 1) * LANES), F32),
            pltpu.VMEM((rings, 2 * rows, LANES), F32),
            pltpu.VMEM((2, rings, 2, blocks, LANES), BF16),
            pltpu.VMEM((2, 2, rings, 2, blocks, LANES), BF16),
            pltpu.VMEM((2, rings, blocks, LANES), BF16),
            pltpu.VMEM((2, lanes_x, rings, blocks, LANES), BF16),
            pltpu.VMEM((blocks, depth, LANES), F32),
            pltpu.VMEM((blocks, depth, LANES), F32),
            pltpu.VMEM((blocks, depth, LANES), BF16),
            pltpu.VMEM((2, 4, depth, depth), BF16),
            pltpu.VMEM((2, depth, depth), BF16),
            pltpu.VMEM((2, depth, depth), BF16),
            pltpu.VMEM((2, 3, depth, LANES), F32),
            pltpu.VMEM((size, size), BF16),
            pltpu.VMEM((size, size), BF16),
            pltpu.VMEM((2, size, size), BF16),
            pltpu.VMEM((2, size, 2 * size), BF16),
            pltpu.VMEM((size, cols), BF16),
            dma((len(operands),)),
            dma((1,)),
            dma((rings,)),
            dma((2, 2)),
            dma((2,)),
            dma((2, groups)),
            dma((3,)),
            dma((3,)),
            dma((2, 2)),
        ],
        compiler_params=pltpu.CompilerParams(collective_id=0, has_side_effects=True),
        name="triangles",
    )(*operands)


def solution(mesh):
    rows = P(("crops", "dap"))
    placed = (P(("crops", "dap"), None, None), P(("crops", "dap"), None), rows, rows) + (P(),) * 12
    return jax.shard_map(
        body, mesh=mesh, in_specs=placed, out_specs=P(("crops", "dap"), None, None), check_vma=False
    )
```

```python
import functools

import jax
import jax.numpy as jnp
from jax import lax
from jax.experimental import pallas as pl
from jax.experimental.pallas import tpu as pltpu
from jax.sharding import PartitionSpec as P

F32 = jnp.float32
BF16 = jnp.bfloat16
MESH = pl.DeviceIdType.MESH
EPS = 1e-05
LANES = 128
GROUP = 8
STRIDE = 4
TAIL = 29
EARLY = 1


def selection(shape, column_of_row):
    rows = lax.broadcasted_iota(jnp.int32, shape, 0)
    columns = lax.broadcasted_iota(jnp.int32, shape, 1)
    return jnp.where(columns == column_of_row(rows), 1.0, 0.0).astype(BF16)


def nn(a, b):
    return lax.dot_general(a, b, (((1,), (0,)), ((), ())), preferred_element_type=F32)


def nt(a, b):
    return lax.dot_general(a, b, (((1,), (1,)), ((), ())), preferred_element_type=F32)


def norm_rows(values):
    scale = 1.0 / values.shape[0]
    center = values - jnp.sum(values, axis=0, keepdims=True) * scale
    spread = jnp.sum(center * center, axis=0, keepdims=True) * scale
    return center * lax.rsqrt(spread + EPS)


class Phases:
    def __init__(self):
        self.scope = None

    def __call__(self, name):
        if self.scope is not None:
            self.scope.__exit__(None, None, None)
        self.scope = jax.named_scope(name) if name else None
        if self.scope is not None:
            self.scope.__enter__()


def column(row_vector):
    return jnp.transpose(jnp.broadcast_to(row_vector, (LANES, LANES)))


def kernel(
    rings,
    lanes_x,
    prior_hbm,
    single_hbm,
    target_hbm,
    mask_hbm,
    recycle_gain_hbm,
    recycle_bias_hbm,
    left_single_hbm,
    right_single_hbm,
    left_target_hbm,
    right_target_hbm,
    tri_gain_hbm,
    tri_proj_hbm,
    tri_gate_hbm,
    tri_gate_bias_hbm,
    tri_out_gain_hbm,
    tri_out_hbm,
    out_ref,
    prior_ref,
    single_ref,
    target_ref,
    mask_ref,
    recycle_gain_ref,
    recycle_bias_ref,
    left_single_ref,
    right_single_ref,
    left_target_ref,
    right_target_ref,
    tri_gain_ref,
    tri_proj_ref,
    tri_gate_ref,
    tri_gate_bias_ref,
    tri_out_gain_ref,
    tri_out_ref,
    terms,
    right_all,
    edges_out,
    edges_in,
    product_out,
    product_in,
    base,
    pair,
    normed,
    weights,
    gate_weights,
    out_weights,
    columns,
    perm,
    perm_back,
    pick,
    pick_right,
    pick_left,
    load_sem,
    terms_send,
    terms_recv,
    edge_sem,
    back_send,
    back_recv,
    twin_send,
    twin_recv,
    lane_sem,
):
    rows, cols, depth = prior_ref.shape
    blocks = rows * cols // LANES
    per_row = cols // LANES
    width = depth // lanes_x
    size = rings * blocks
    dap = lax.axis_index("dap")
    x = lax.axis_index("chan")
    z = dap // 2
    h = lax.rem(dap, 2)
    twin = {"dap": dap + 1 - 2 * h}
    phase = Phases()

    def offset(p):
        up = (p + 1) // 2
        return rings + up * (2 * lax.rem(p, 2) - 1)

    def to_z(peer):
        return {"dap": 2 * peer + h}

    def to_x(t):
        return lax.rem(x + t, lanes_x)

    phase("greet")
    barrier = pltpu.get_barrier_semaphore()

    q = lax.rem(z + rings - 1, rings)
    last = rings - 1

    def at(order):
        return {"dap": 2 * lax.rem(order + 1, rings) + 1 - h}

    def greet(order):
        pl.semaphore_signal(barrier, inc=1, device_id=at(order), device_id_type=MESH)

    for back in range(1, STRIDE + 1):
        pl.when(q >= back)(functools.partial(greet, q - back))
    pl.semaphore_signal(barrier, inc=1, device_id=twin, device_id_type=MESH)
    for t in range(1, lanes_x):
        pl.semaphore_signal(barrier, inc=1, device_id={"chan": to_x(t)}, device_id_type=MESH)

    sources = (
        (single_hbm, single_ref),
        (right_single_hbm, right_single_ref),
        (target_hbm, target_ref),
        (mask_hbm, mask_ref),
        (right_target_hbm, right_target_ref),
        (left_single_hbm, left_single_ref),
        (left_target_hbm, left_target_ref),
        (recycle_gain_hbm, recycle_gain_ref),
        (recycle_bias_hbm, recycle_bias_ref),
        (prior_hbm, prior_ref),
        (tri_proj_hbm, tri_proj_ref),
        (tri_gain_hbm, tri_gain_ref),
        (tri_gate_hbm, tri_gate_ref),
        (tri_gate_bias_hbm, tri_gate_bias_ref),
        (tri_out_gain_hbm, tri_out_gain_ref),
        (tri_out_hbm, tri_out_ref),
    )
    loads = [
        pltpu.make_async_copy(source, held, load_sem.at[n])
        for n, (source, held) in enumerate(sources)
    ]
    for load in loads:
        load.start()

    def greet_later(order, carry):
        greet(order)
        return carry

    lax.fori_loop(q + 1, rings, greet_later, 0)

    phase("terms")
    for load in loads[:5]:
        load.wait()
    single = single_ref[...]
    mask_of = [mask_ref[r].astype(F32) for r in range(rows)]

    def row_terms(weight_ref, table_ref):
        linear = nn(single, weight_ref[...])
        table = table_ref[...].astype(F32)
        classes = lax.broadcasted_iota(jnp.int32, table.shape, 0)
        picked = [
            jnp.sum(jnp.where(classes == target_ref[r], table, 0.0), axis=0, keepdims=True)
            for r in range(rows)
        ]
        return [linear[r : r + 1] + picked[r] for r in range(rows)]

    right_rows = row_terms(right_single_ref, right_target_ref)
    lane_row = lax.rem(lax.broadcasted_iota(jnp.int32, (1, LANES), 1), rows)
    mask_row = jnp.zeros((1, LANES), F32)
    for r in range(rows):
        mask_row = jnp.where(lane_row == r, mask_of[r], mask_row)
    for r, row in enumerate(right_rows + [mask_row]):
        terms[h, z, :, r * LANES : (r + 1) * LANES] = row

    phase("barrier")
    pl.semaphore_wait(barrier, q + jnp.minimum(STRIDE, last - q) + 1 + lanes_x - 1)

    def remote(source, target, send, recv, device):
        return pltpu.make_async_remote_copy(
            src_ref=source,
            dst_ref=target,
            send_sem=send,
            recv_sem=recv,
            device_id=device,
            device_id_type=MESH,
        )

    closing = []
    starts = [*range(1, TAIL, GROUP), TAIL]
    spans = list(zip(starts, starts[1:] + [rings]))

    def group_of(p):
        return (p - 1) // GROUP + jnp.where(p >= TAIL, 1, 0)

    phase("tsend")

    def give(source, order):
        tile, landing = terms.at[h, source], terms.at[1 - h, source]
        remote(tile, landing, terms_send.at[0], terms_recv.at[source], at(order)).start()

    def carried(source):
        return lax.rem(source, lanes_x) == x

    for ahead in range(1, STRIDE + 1):
        pl.when(carried(z) & (q + ahead <= last))(functools.partial(give, z, q + ahead))

    def give_earlier(t, carry):
        order = lax.rem(q + offset(rings - 1 - t), rings)
        pl.when(order < q)(functools.partial(give, z, order))
        return carry

    lax.fori_loop(0, rings - 1, give_earlier, 0)

    def await_terms(source):
        tile = terms.at[h, source]
        remote(tile, tile, terms_send.at[0], terms_recv.at[source], twin).wait_recv()

    early = q + STRIDE <= last

    def lower(order):
        return lax.rem(order + 1, rings)

    def hand_over(source):
        tile = terms.at[h, source]
        for lane in range(1, lanes_x):
            to = {"chan": to_x(lane)}
            remote(tile, tile, terms_send.at[0], terms_recv.at[source], to).start()

    def relay(order, carry):
        source = lower(order)

        @pl.when(carried(source))
        def _():
            await_terms(source)
            pl.when(early)(functools.partial(give, source, q + STRIDE))
            pl.when(jnp.logical_not(early))(functools.partial(hand_over, source))

        return carry

    def hand_over_all(order, carry):
        source = lower(order)
        pl.when(carried(source))(functools.partial(hand_over, source))
        return carry

    def relay_all():
        lax.fori_loop(0, q, relay, 0)
        lax.fori_loop(0, jnp.where(early, q, 0), hand_over_all, 0)

    def collect(order, carry):
        source = lower(order)
        pl.when(jnp.logical_not(carried(source)))(functools.partial(await_terms, source))
        return carry

    def prepare():
        for load in loads[5:]:
            load.wait()
        left_rows = row_terms(left_single_ref, left_target_ref)
        gain = recycle_gain_ref[...]
        bias = recycle_bias_ref[...]
        for r in range(rows):
            for jh in range(per_row):
                block = prior_ref[r, jh * LANES : (jh + 1) * LANES, :].astype(F32)
                center = block - jnp.mean(block, axis=1, keepdims=True)
                spread = jnp.mean(center * center, axis=1, keepdims=True)
                value = center * lax.rsqrt(spread + EPS) * gain + bias + left_rows[r]
                base[r * per_row + jh] = jnp.transpose(value)
        for u in range(2):
            whole = tri_proj_ref[u].astype(F32)
            for g in range(4):
                weights[u, g] = jnp.transpose(whole[:, g, :]).astype(BF16)
            gate_weights[u] = jnp.transpose(tri_gate_ref[u].astype(F32)).astype(BF16)
            out_weights[u] = jnp.transpose(tri_out_ref[u].astype(F32)).astype(BF16)
            columns[u, 0] = column(tri_gain_ref[u : u + 1, :])
            columns[u, 1] = column(tri_gate_bias_ref[u : u + 1, :])
            columns[u, 2] = column(tri_out_gain_ref[u : u + 1, :])

        def place(channel):
            delta = lax.rem(channel - z + rings, rings)
            after = jnp.where(delta <= rings // 2, 2 * delta - 1, 2 * (rings - delta))
            return jnp.where(delta == 0, 0, after)

        perm[...] = selection((size, size), lambda q: lax.rem(q, blocks) * rings + q // blocks)
        perm_back[...] = selection(
            (size, size), lambda q: place(lax.rem(q, rings)) * blocks + q // rings
        )
        for half in range(2):
            pick[half] = selection((size, size), lambda q: q - lax.rem(q, 2) + half)
            pick_right[half] = selection(
                (size, 2 * size),
                lambda j: lax.rem(j // rows, 2) * size
                + (j // (2 * rows)) * blocks
                + 2 * lax.rem(j, rows)
                + half,
            )
        pick_left[...] = selection(
            (size, cols), lambda q: (q // blocks) * 2 * rows + rows * h + lax.rem(q, blocks) // 2
        )

    phase("relay")

    def turn(step, carry):
        pl.when((step == 0) == early)(relay_all)
        pl.when((step == 1) == early)(prepare)
        return carry

    lax.fori_loop(0, 2, turn, 0)

    phase("twait")
    def later(order, carry):
        await_terms(lax.rem(order + 1, rings))
        return carry

    lax.fori_loop(0, q, collect, 0)
    lax.fori_loop(q + 1, rings, later, 0)
    phase("ttwin")

    def swap(view, k):
        def copy(parity):
            return remote(view(parity), view(parity), twin_send.at[k], twin_recv.at[k], twin)

        copy(h).start()
        closing.append(copy(h).wait_send)
        copy(1 - h).wait_recv()

    swap(lambda parity: terms.at[parity], 0)

    phase("pair")
    source = lax.broadcasted_iota(jnp.int32, (rings, LANES), 0)
    order = lax.rem(source + rings - 1, rings)
    even = lax.rem((q - order - 1 + rings * STRIDE) // STRIDE, 2) == rings % 2
    same = (order == q) | ((order < q) & jnp.logical_not(even))

    def of_parity(parity, r):
        got = [terms[core, :, 0, r * LANES : (r + 1) * LANES] for core in range(2)]
        return jnp.where(same, got[parity], got[1 - parity])

    for parity in range(2):
        for r in range(rows):
            right_all[:, parity * rows + r, :] = of_parity(parity, r)
    right_whole = right_all[...].reshape(cols, depth)
    lane = lax.broadcasted_iota(jnp.int32, (rings, LANES), 1)
    first, second = (of_parity(parity, rows) for parity in range(2))
    mask_table = jnp.where(lax.rem(lane // rows, 2) == 0, first, second)
    masks = []
    for jh in range(per_row):
        right_t = jnp.transpose(right_whole[jh * LANES : (jh + 1) * LANES])
        chosen = source == (jh * LANES + lane) // (2 * rows)
        masks.append(jnp.sum(jnp.where(chosen, mask_table, 0.0), axis=0, keepdims=True))
        for r in range(rows):
            m = r * per_row + jh
            pair[m] = (base[m] + right_t).astype(BF16).astype(F32)

    for u in range(2):
        phase("edges")
        local = [
            weights[u, g, pl.ds(pl.multiple_of(x * width, width), width), :] for g in range(4)
        ]
        local = jnp.concatenate(local, axis=0)
        left_parts, right_parts = [], []
        for m in range(blocks):
            block = (norm_rows(pair[m]) * columns[u, 0]).astype(BF16)
            normed[m] = block
            projected = nn(local, block)
            masked = masks[m % per_row] * mask_of[m // per_row]
            value, gate = projected[:width], projected[width : 2 * width]
            left_parts.append((masked * jax.nn.sigmoid(gate) * value).astype(BF16))
            value, gate = projected[2 * width : 3 * width], projected[3 * width :]
            right_parts.append((masked * jax.nn.sigmoid(gate) * value).astype(BF16))
        for side, parts in enumerate((left_parts, right_parts)):
            ordered = nn(perm[...], jnp.concatenate(parts, axis=0)).astype(BF16)
            edges_out[u, :, side] = ordered.reshape(rings, blocks, LANES)

        phase("esend")

        def send_edges(t, carry, u=u):
            peer = lax.rem(z + offset(rings - 1 - t), rings)
            remote(
                edges_out.at[u, peer],
                edges_in.at[u, h, z],
                edge_sem.at[u, 0],
                edge_sem.at[u, 1],
                to_z(peer),
            ).start()
            return carry

        lax.fori_loop(0, rings - 1, send_edges, 0)
        edges_in[u, h, z] = edges_out[u, z]
        gating = [
            jax.nn.sigmoid(nn(gate_weights[u], normed[m]) + columns[u, 1]) for m in range(blocks)
        ]
        many = edges_in.at[u, h, pl.ds(0, rings - 1)]
        edges_all = remote(many, many, edge_sem.at[u, 0], edge_sem.at[u, 1], twin)
        closing.append(edges_all.wait_send)
        if u == 0:
            relayed = (q - x + lanes_x) // lanes_x - jnp.where(x == 0, 1, 0)
            copies = lanes_x - 1 + jnp.where(q + STRIDE <= last, 1, 0)
            ahead = jnp.where(carried(z), jnp.minimum(STRIDE, last - q), 0)
            given = ahead + q + relayed * copies

            def gone(t, carry):
                tile = terms.at[h, z]
                remote(tile, tile, terms_send.at[0], terms_recv.at[z], twin).wait_send()
                return carry

            lax.fori_loop(0, given, gone, 0)
        phase("ewait")
        edges_all.wait_recv()
        phase("etwin")
        if u == 0:
            swap(lambda parity: edges_in.at[0, parity, :, 1], 1)
        else:
            swap(lambda parity: edges_in.at[1, parity], 2)

        phase("product")
        right_rows_all = edges_in[u, :, :, 1].reshape(2 * size, LANES)
        if u == 0:
            left_own = edges_in[u, h, :, 0].reshape(size, LANES)
            a = [nn(pick[half], left_own).astype(BF16) for half in range(2)]
            b = [nn(pick_right[half], right_rows_all).astype(BF16) for half in range(2)]
            whole = nt(jnp.concatenate(a, axis=1), jnp.concatenate(b, axis=1))
            even = lax.rem(lax.broadcasted_iota(jnp.int32, (size, LANES), 0), 2) == 0
            product = jnp.where(even, whole[:, :LANES], whole[:, LANES:])
        else:
            spread = []
            for parity in range(2):
                block = edges_in[u, parity, :, 0].reshape(size, LANES)
                halves = [nn(pick[half], block).astype(BF16) for half in range(2)]
                spread.append(jnp.concatenate(halves, axis=1))
            chosen = nt(pick_left[...], jnp.concatenate(spread, axis=0))
            row_half = lax.rem(lax.broadcasted_iota(jnp.int32, chosen.shape, 0), 2)
            column_half = lax.rem(lax.broadcasted_iota(jnp.int32, chosen.shape, 1), 2)
            chosen = jnp.where(row_half == column_half, chosen, 0.0).astype(BF16)
            product = nn(chosen, right_rows_all)
        product_out[u] = product.astype(BF16).reshape(rings, blocks, LANES)

        phase("bsend")

        def send_back(t, carry, u=u):
            p = rings - 1 - t
            peer = lax.rem(z + 2 * rings - offset(p), rings)

            def send(lane):
                remote(
                    product_out.at[u, peer],
                    product_in.at[u, x, p],
                    back_send.at[u],
                    lane_sem.at[u, 1] if lane else back_recv.at[u, group_of(p)],
                    {"dap": 2 * peer + h, "chan": to_x(lane)} if lane else to_z(peer),
                ).start()

            send(0)
            if u:

                @pl.when(peer < EARLY)
                def _():
                    for lane in range(1, lanes_x):
                        send(lane)

            return carry

        lax.fori_loop(0, rings - 1, send_back, 0)
        product_in[u, x, 0] = product_out[u, z]
        phase("bwait")
        direct = z < EARLY

        def forward(part, u=u):
            for t in (2, 1, 3) if lanes_x == 4 else range(1, lanes_x):
                remote(part, part, lane_sem.at[u, 0], lane_sem.at[u, 1], {"chan": to_x(t)}).start()

        def sent_back(many, times, u=u):
            def gone(t, carry):
                remote(many, many, back_send.at[u], back_recv.at[u, 0], twin).wait_send()
                return carry

            return functools.partial(lax.fori_loop, 0, times, gone, 0)

        closing.append(sent_back(product_out.at[u, pl.ds(0, rings - 1)], 1))
        if u:
            elsewhere = EARLY - jnp.where(direct, 1, 0)
            closing.append(sent_back(product_out.at[u, 0], elsewhere * (lanes_x - 1)))
            pl.when(direct)(functools.partial(forward, product_in.at[u, x, 0]))
        for g, (start, stop) in enumerate(spans):
            arrived = product_in.at[u, x, pl.ds(start, stop - start)]
            remote(arrived, arrived, back_send.at[u], back_recv.at[u, g], twin).wait_recv()
            begin = start if g else 0
            part = product_in.at[u, x, pl.ds(begin, stop - begin)]
            if u:
                pl.when(jnp.logical_not(direct))(functools.partial(forward, part))
            else:
                forward(part)
        phase("lwait")
        many = product_in.at[u, pl.ds(0, lanes_x - 1)]
        remote(many, many, lane_sem.at[u, 0], lane_sem.at[u, 1], twin).wait_recv()

        def sent_on(count, u=u):
            many = product_in.at[u, pl.ds(0, lanes_x - 1), pl.ds(0, count)]
            remote(many, many, lane_sem.at[u, 0], lane_sem.at[u, 1], twin).wait_send()

        one_sent, all_sent = functools.partial(sent_on, 1), functools.partial(sent_on, rings)
        if u:
            closing.append(functools.partial(pl.when(direct), one_sent))
            closing.append(functools.partial(pl.when(jnp.logical_not(direct)), all_sent))
        else:
            closing.append(all_sent)

        phase("hidden")
        hidden = [
            nn(perm_back[...], product_in[u, lane].reshape(size, LANES)) for lane in range(lanes_x)
        ]
        for m in range(blocks):
            block = jnp.concatenate([part[m * rings : (m + 1) * rings] for part in hidden], axis=0)
            block = (norm_rows(block) * columns[u, 2]).astype(BF16)
            update = nn(out_weights[u], block)
            value = pair[m] + gating[m] * update
            if u == 0:
                pair[m] = value.astype(BF16).astype(F32)
            else:
                r, jh = m // per_row, m % per_row
                out_ref[r, jh * LANES : (jh + 1) * LANES, :] = jnp.transpose(value).astype(BF16)

    phase("close")
    for wait in closing:
        wait()
    phase(None)


def body(
    prior_pair,
    single,
    target,
    residue_mask,
    recycle_gain,
    recycle_bias,
    left_single,
    right_single,
    left_target,
    right_target,
    tri_gain,
    tri_proj,
    tri_gate,
    tri_gate_bias,
    tri_out_gain,
    tri_out,
):
    rings = lax.axis_size("dap") // 2
    lanes_x = lax.axis_size("chan")
    rows, cols, depth = prior_pair.shape
    blocks = rows * cols // LANES
    size = rings * blocks
    groups = -(-(TAIL - 1) // GROUP) + 1
    vmem = pl.BlockSpec(memory_space=pltpu.VMEM)
    hbm = pl.BlockSpec(memory_space=pltpu.HBM)
    dma = pltpu.SemaphoreType.DMA
    operands = (
        prior_pair,
        single,
        target,
        residue_mask,
        recycle_gain[None, :],
        recycle_bias[None, :],
        left_single,
        right_single,
        left_target,
        right_target,
        tri_gain,
        tri_proj,
        tri_gate,
        tri_gate_bias,
        tri_out_gain,
        tri_out,
    )
    held = [
        pltpu.SMEM(a.shape, a.dtype) if a.dtype == jnp.int32 else pltpu.VMEM(a.shape, a.dtype)
        for a in operands
    ]
    return pl.pallas_call(
        functools.partial(kernel, rings, lanes_x),
        out_shape=pltpu.VMEM(prior_pair.shape, BF16),
        in_specs=[hbm] * len(operands),
        out_specs=vmem,
        scratch_shapes=held
        + [
            pltpu.VMEM((2, rings, 1, (rows + 1) * LANES), F32),
            pltpu.VMEM((rings, 2 * rows, LANES), F32),
            pltpu.VMEM((2, rings, 2, blocks, LANES), BF16),
            pltpu.VMEM((2, 2, rings, 2, blocks, LANES), BF16),
            pltpu.VMEM((2, rings, blocks, LANES), BF16),
            pltpu.VMEM((2, lanes_x, rings, blocks, LANES), BF16),
            pltpu.VMEM((blocks, depth, LANES), F32),
            pltpu.VMEM((blocks, depth, LANES), F32),
            pltpu.VMEM((blocks, depth, LANES), BF16),
            pltpu.VMEM((2, 4, depth, depth), BF16),
            pltpu.VMEM((2, depth, depth), BF16),
            pltpu.VMEM((2, depth, depth), BF16),
            pltpu.VMEM((2, 3, depth, LANES), F32),
            pltpu.VMEM((size, size), BF16),
            pltpu.VMEM((size, size), BF16),
            pltpu.VMEM((2, size, size), BF16),
            pltpu.VMEM((2, size, 2 * size), BF16),
            pltpu.VMEM((size, cols), BF16),
            dma((len(operands),)),
            dma((1,)),
            dma((rings,)),
            dma((2, 2)),
            dma((2,)),
            dma((2, groups)),
            dma((3,)),
            dma((3,)),
            dma((2, 2)),
        ],
        compiler_params=pltpu.CompilerParams(collective_id=0, has_side_effects=True),
        name="triangles",
    )(*operands)


def solution(mesh):
    rows = P(("crops", "dap"))
    placed = (P(("crops", "dap"), None, None), P(("crops", "dap"), None), rows, rows) + (P(),) * 12
    return jax.shard_map(
        body, mesh=mesh, in_specs=placed, out_specs=P(("crops", "dap"), None, None), check_vma=False
    )
```
